32 devices in a mesh: row: 4 (over y, x), col: 8 (over z, core).
Axes of the slice: x: 2, y: 2, z: 4, core: 2. Of those that a mesh axis runs over, the one named last changes fastest.
Arguments:
- features: bfloat16 [8192, 512], P(('row', 'col')), may hold values from -6 to 6
- tile_values: bfloat16 [4, 8, 128, 128, 128], P('row', 'col'), may hold values from -0.1875 to 0.1875
- tile_places: int32 [4, 8, 2, 128], P('row', 'col'), may hold values from 0 to 15, as said below
- tile_counts: int32 [4, 8], replicated, may hold values from 40 to 128, as said below
- weight_one: float32 [512, 512], replicated, may hold values from -0.25 to 0.25
- weight_two: float32 [512, 512], replicated, may hold values from -0.25 to 0.25
Outputs:
- embedded: float32 [8192, 512], P(('row', 'col'))
The draws below stay inside these ranges and needn't reach their ends.
Inputs may be any that keep to these rules, and one draw needn't show every extreme that they name: `tile_places`: in every block the first tile_counts slots name distinct tiles with tile rows below 16 and tile columns below 8, listed in order of tile row (never falling); later slots also name tiles in range. `tile_counts`: some block has exactly 128 tiles.
All inputs are finite; a program needn't handle non-finite values.
Results may differ from the reference program's by a relative error of at most 0.0029.
Values may be sent and summed in bfloat16 or wider, within the bound.
A program may use at most 64 MiB of HBM per device.

```python
import jax
import jax.numpy as jnp
from jax import lax

F = 512
TILE = 128
TR = 16
TC = 8
MAXT = 128
LOW = 40
PIECE = 256
ITEMS = 8192
N_ROW = 4
N_COL = 8


def block_counts(key):
    base_key = jax.random.fold_in(key, 11)
    first_key, second_key = jax.random.split(base_key)
    counts = jax.random.randint(first_key, (N_ROW * N_COL,), LOW, MAXT + 1)
    fullest = jax.random.randint(second_key, (), 0, N_ROW * N_COL)
    counts = jnp.where(jnp.arange(N_ROW * N_COL) == fullest, MAXT, counts)
    return counts.astype(jnp.int32)


def draw_tile_places(key, part):
    counts = block_counts(key)
    device_keys = jax.random.split(jax.random.fold_in(key, 23), N_ROW * N_COL)

    def draw_one(device_key, count):
        ordering = jax.random.permutation(device_key, TR * TC)[:MAXT]
        slots = jnp.arange(MAXT)
        keyed = jnp.where(slots < count, ordering, ordering + TR * TC)
        ranked = jnp.sort(keyed)
        chosen = jnp.where(ranked >= TR * TC, ranked - TR * TC, ranked)
        return jnp.stack([chosen // TC, chosen % TC]).astype(jnp.int32)
    return jax.vmap(draw_one)(device_keys, counts).reshape(N_ROW, N_COL, 2, MAXT)


def draw_tile_counts(key, part):
    return block_counts(key).reshape(N_ROW, N_COL)


def shard_levels(rng, dims, cuts, least, top_value):
    def one(axis_at, parts):
        heights = jax.random.uniform(jax.random.fold_in(jax.random.fold_in(rng, 6), axis_at), (parts,), jnp.float32, least / len(cuts), top_value / len(cuts))
        return jnp.repeat(jnp.exp(heights), dims[axis_at] // parts).reshape((-1,) + (1,) * (len(dims) - axis_at - 1))

    factor_of = one(*cuts[0])
    for cut in cuts[1:]:
        factor_of = factor_of * one(*cut)
    return factor_of


def scatter_about(rng, shape, width, reach, shards=(), held_as=jnp.bfloat16):
    result = jax.random.normal(rng, shape, jnp.float32) * width
    if len(shards) > 0:
        result = shard_levels(rng, shape, shards, -0.22, 0.18) * result
    return jnp.clip(result, min=-reach, max=reach).astype(held_as)


def setup_inputs(seed: int = 0) -> dict:
    splits = jax.random.split(jax.random.key(seed), 7)
    return {
        "features": scatter_about(splits[0], (ITEMS, F), 1.0, 6.0, ((0, 32),)),
        "tile_values": scatter_about(splits[1], (N_ROW, N_COL, MAXT, TILE, TILE), (MAXT * TILE // TR) ** -0.5, 0.1875, ((0, 4), (1, 8))),
        "tile_places": draw_tile_places(jax.random.fold_in(splits[6], 71), 0),
        "tile_counts": draw_tile_counts(jax.random.fold_in(splits[6], 71), 0),
        "weight_one": scatter_about(splits[4], (F, F), F ** -0.5, 0.25, (), jnp.float32),
        "weight_two": scatter_about(splits[5], (F, F), F ** -0.5, 0.25, (), jnp.float32),
    }


def aggregate(tile_values, tile_places, tile_counts, inputs):
    feature_blocks = inputs.reshape(N_ROW, N_COL, PIECE, F)
    all_values = tile_values.reshape(N_ROW * N_COL, MAXT, TILE, TILE)
    all_places = tile_places.reshape(N_ROW * N_COL, 2, MAXT)
    all_counts = tile_counts.reshape(N_ROW * N_COL)

    def one_block(totals, device_id):
        block_row = device_id // N_COL
        block_col = device_id % N_COL
        gathered = lax.dynamic_index_in_dim(feature_blocks, block_col, 1, keepdims=False)
        column_tiles = gathered.reshape(TC, TILE, F).astype(jnp.float32)
        blocks = all_values[device_id].astype(jnp.float32)
        places = all_places[device_id]
        active = (jnp.arange(MAXT, dtype=jnp.int32) < all_counts[device_id]).astype(jnp.float32)
        products = jnp.einsum("sij,sjf->sif", blocks, column_tiles[places[1]]) * active[:, None, None]
        partial_value = jnp.zeros((TR, TILE, F), jnp.float32).at[places[0]].add(products)
        return totals.at[block_row].add(partial_value), None

    start_totals = jnp.zeros((N_ROW, TR, TILE, F), jnp.float32)
    totals, _ = lax.scan(one_block, start_totals, jnp.arange(N_ROW * N_COL, dtype=jnp.int32))
    return totals.reshape(ITEMS, F)


def reference(features, tile_values, tile_places, tile_counts, weight_one, weight_two):
    first = aggregate(tile_values, tile_places, tile_counts, features)
    hidden = jnp.maximum(jnp.dot(first, weight_one, precision=lax.Precision.HIGHEST), 0.0).astype(jnp.bfloat16)
    second = aggregate(tile_values, tile_places, tile_counts, hidden)
    return jnp.maximum(jnp.dot(second, weight_two, precision=lax.Precision.HIGHEST), 0.0)
```

```python
import functools

import jax
import jax.numpy as jnp
from jax import lax
from jax.experimental import pallas as pl
from jax.experimental.pallas import tpu as pltpu
from jax.sharding import PartitionSpec as P

MESH = pl.DeviceIdType.MESH
PARTS = 4
LINK_TYPES = (jnp.int16, jnp.bfloat16)
TOP = 32766.0
SKEW = 3
LEAD = 2


def kernel(
    n_row, n_col, blocks,
    counts_hbm, places_hbm, features_hbm, tiles_hbm, weight_one_hbm, weight_two_hbm,
    out_hbm,
    tiles, dense, weights, inputs, total, result, prod, pair_in,
    up_out0, up_in0, down_out0, down_in0, up_out1, up_in1, down_out1, down_in1,
    scale_out, scale_in,
    load_sem, feature_sem, out_sem, near_send, near_recv, far_send, far_recv, pair_send, pair_recv,
    flow_send_sem, flow_recv_sem, scale_send, scale_recv,
    counts, places, inverse_rows, inverse_ref,
):
    row, col = lax.axis_index("row"), lax.axis_index("col")
    n_chip = n_col // 2
    chip, core = col // 2, col % 2
    partner = chip * 2 + (1 - core)
    slots, tile = tiles_hbm.shape[0], tiles_hbm.shape[1]
    piece, width = features_hbm.shape
    part = width // PARTS
    sub = piece // blocks
    depth = piece * n_row
    tile_rows, tile_cols = dense.shape[0] // tile, depth // tile
    turns = n_chip - 1
    first = PARTS * turns
    steps = blocks * first
    bits = [1 << i for i in range((n_row - 1).bit_length())]
    masks = sorted((m for m in range(1, n_row) if m & (m - 1)), key=lambda m: bin(m).count("1"))

    barrier = pltpu.get_barrier_semaphore()
    for bit in bits:
        pl.semaphore_signal(barrier, inc=1, device_id=(row ^ bit, col), device_id_type=MESH)
    pl.semaphore_signal(barrier, inc=1, device_id=(row, partner), device_id_type=MESH)

    @pl.when(chip > 0)
    def _():
        pl.semaphore_signal(barrier, inc=1, device_id=(row, col - 2), device_id_type=MESH)

    @pl.when(chip < n_chip - 1)
    def _():
        pl.semaphore_signal(barrier, inc=1, device_id=(row, col + 2), device_id_type=MESH)

    def slot_rows(b, q):
        return pl.ds(pl.multiple_of((b * n_row + q) * sub, sub), sub)

    feature_loads = [
        [
            pltpu.make_async_copy(
                features_hbm.at[pl.ds(b * sub, sub), pl.ds(h * part, part)],
                inputs.at[0, h, slot_rows(b, row), :],
                feature_sem.at[b, h],
            )
            for b in range(blocks)
        ]
        for h in range(PARTS)
    ]
    for loads in feature_loads:
        for load in loads:
            load.start()
    counts_load = pltpu.make_async_copy(counts_hbm, counts, load_sem.at[4])
    counts_load.start()
    places_load = pltpu.make_async_copy(places_hbm, places, load_sem.at[5])
    places_load.start()
    tile_load = pltpu.make_async_copy(tiles_hbm, tiles.at[pl.ds(0, slots)], load_sem.at[0])
    tile_load.start()
    weight_loads = [
        pltpu.make_async_copy(weight_one_hbm, weights.at[0], load_sem.at[1]),
        pltpu.make_async_copy(weight_two_hbm, weights.at[1], load_sem.at[2]),
    ]
    for load in weight_loads:
        load.start()

    peers = len(bits) + 1 + jnp.where(chip > 0, 1, 0) + jnp.where(chip < n_chip - 1, 1, 0)

    def near_copy(layer, b, h, i):
        block = inputs.at[layer, h, slot_rows(b, row), :]
        return pltpu.make_async_remote_copy(
            src_ref=block, dst_ref=block,
            send_sem=near_send.at[layer, b, h, i], recv_sem=near_recv.at[layer, b, h, i],
            device_id=(row ^ bits[i], col), device_id_type=MESH,
        )

    half = sub // 2

    def far_copy(layer, b, h, i, side):
        mask = masks[i]
        last = 1 << (mask.bit_length() - 1) if side == 0 else mask & -mask
        origin = row ^ (mask ^ last)
        rows = pl.ds(pl.multiple_of((b * n_row + origin) * sub + side * half, half), half)
        block = inputs.at[layer, h, rows, :]
        return pltpu.make_async_remote_copy(
            src_ref=block, dst_ref=block,
            send_sem=far_send.at[layer, b, h, i, side], recv_sem=far_recv.at[layer, b, h, i, side],
            device_id=(row ^ last, col), device_id_type=MESH,
        )

    def near_start(layer, some, h):
        for b in some:
            for i in range(len(bits)):
                near_copy(layer, b, h, i).start()

    def far_start(layer, some, h, level):
        for b in some:
            for i, mask in enumerate(masks):
                if bin(mask).count("1") == level:
                    for side in (0, 1):
                        far_copy(layer, b, h, i, side).start()

    def relay(layer, some, h):
        for b in some:
            for i in range(len(bits)):
                near_copy(layer, b, h, i).wait_recv()
        far_start(layer, some, h, 2)

    def arrive(layer, some, h):
        for level in range(2, len(bits) + 1):
            for b in some:
                for i, mask in enumerate(masks):
                    if bin(mask).count("1") == level:
                        for side in (0, 1):
                            far_copy(layer, b, h, i, side).wait_recv()
            if level < len(bits):
                far_start(layer, some, h, level + 1)

    def pair_copy(layer, h, d):
        return pltpu.make_async_remote_copy(
            src_ref=prod.at[layer, h, d, 1 - core],
            dst_ref=pair_in.at[layer, h, d],
            send_sem=pair_send.at[layer, h, d], recv_sem=pair_recv.at[layer, h, d],
            device_id=(row, partner), device_id_type=MESH,
        )

    flows = (
        ((up_out0, up_in0), (down_out0, down_in0)),
        ((up_out1, up_in1), (down_out1, down_in1)),
    )

    def flow_copy(layer, way, k):
        out_buffer, in_buffer = flows[layer][way]
        return pltpu.make_async_remote_copy(
            src_ref=out_buffer.at[k], dst_ref=in_buffer.at[k],
            send_sem=flow_send_sem.at[layer, way, k], recv_sem=flow_recv_sem.at[layer, way, k],
            device_id=(row, col + 2 if way == 0 else col - 2), device_id_type=MESH,
        )

    def scale_copy(way, k):
        return pltpu.make_async_remote_copy(
            src_ref=scale_out.at[way, k], dst_ref=scale_in.at[way, k],
            send_sem=scale_send.at[way, k], recv_sem=scale_recv.at[way, k],
            device_id=(row, col + 2 if way == 0 else col - 2), device_id_type=MESH,
        )

    def flow_send(layer, way, k, value):
        target = flows[layer][way][0]
        if LINK_TYPES[layer] == jnp.int16:
            peak = jnp.maximum(jnp.max(jnp.abs(value), axis=0, keepdims=True), 1e-30)
            scale_out[way, k] = peak * (1.0 / TOP)
            scale_copy(way, k).start()
            target[k] = jnp.round(value * (TOP / peak)).astype(jnp.int32).astype(jnp.int16)
        else:
            target[k] = value.astype(target.dtype)
        flow_copy(layer, way, k).start()

    def flow_take(layer, way, k):
        source = flows[layer][way][1]
        flow_copy(layer, way, k).wait_recv()
        if LINK_TYPES[layer] == jnp.int16:
            scale_copy(way, k).wait_recv()
            return source[k].astype(jnp.int32).astype(jnp.float32) * scale_in[way, k]
        return source[k].astype(jnp.float32)

    def pair_sum(layer, b, h, d):
        rows = pl.ds(pl.multiple_of(b * sub, sub), sub)
        return prod[layer, h, d, core, rows, :] + pair_in[layer, h, d, rows, :]

    def place_of(k):
        k = jnp.clip(k, 0, steps - 1)
        later = jnp.maximum(k - first, 0)
        b = jnp.where(k < first, 0, 1 + later // first)
        rest = lax.rem(later, first)
        h = jnp.where(k < first, k // turns, lax.rem(rest, PARTS))
        j = jnp.where(k < first, lax.rem(k, turns), rest // PARTS)
        return b, h, j

    def order_of(b, h, j):
        return h * turns + j if b == 0 else b * first + j * PARTS + h

    def send_step(layer, t):
        for way in (0, 1):
            hops = chip if way == 0 else turns - chip
            k = t - SKEW * hops
            b, h, j = place_of(k)
            d = turns - j if way == 0 else j
            ahead = d > chip if way == 0 else d < chip

            @pl.when((k >= 0) & (k < steps) & ahead)
            def _():
                @pl.when(b == 0)
                def _():
                    pair_copy(layer, h, d).wait_recv()

                @pl.when(hops == 0)
                def _():
                    flow_send(layer, way, k, pair_sum(layer, b, h, d))

                @pl.when(hops > 0)
                def _():
                    flow_send(
                        layer, way, k, pair_sum(layer, b, h, d) + flow_take(layer, way, k)
                    )

    def settle(layer, b):
        for h in range(PARTS):
            columns = slice(h * part, (h + 1) * part)
            if b == 0:
                pair_copy(layer, h, chip).wait_recv()
            total[b, :, columns] = pair_sum(layer, b, h, chip)

            @pl.when(chip > 0)
            def _():
                k = b * first + h + PARTS * (turns - chip) if b else h * turns + turns - chip
                total[b, :, columns] += flow_take(layer, 0, k)

            @pl.when(chip < turns)
            def _():
                k = b * first + h + PARTS * chip if b else h * turns + chip
                total[b, :, columns] += flow_take(layer, 1, k)

    def project(layer, b):
        return jnp.dot(
            total[b], weights[layer], precision=lax.Precision.HIGHEST,
            preferred_element_type=jnp.float32,
        )

    def chip_rows(d):
        return pl.ds(pl.multiple_of(d * (2 * piece), 2 * piece), 2 * piece)

    def unit_chip(i):
        return jnp.where(chip < n_chip // 2, turns - i, i)

    last_depth = depth // blocks
    early = depth - last_depth

    def unit(layer, some, h, i):

        @pl.when(i == 0)
        def _():
            @pl.when(h + 1 < PARTS)
            def _():
                relay(layer, some, h + 1)

            @pl.when(h + 3 < PARTS)
            def _():
                near_start(layer, some, h + 3)

            arrive(layer, some, h)

        d = unit_chip(i)
        if layer == 0 or blocks == 1:
            value = jnp.dot(
                dense[chip_rows(d), :], inputs[layer, h], preferred_element_type=jnp.float32
            )
            prod[layer, h, d] = value.reshape(2, piece, part)
        else:
            value = jnp.dot(
                dense[chip_rows(d), early:], inputs[layer, h, early:, :],
                preferred_element_type=jnp.float32,
            )
            prod[layer, h, d] += value.reshape(2, piece, part)
        pair_copy(layer, h, d).start()

    def early_unit(i):
        d = unit_chip(i)
        known = jnp.concatenate([inputs[1, h, 0:early, :] for h in range(PARTS)], axis=1)
        value = jnp.dot(dense[chip_rows(d), 0:early], known, preferred_element_type=jnp.float32)
        for h in range(PARTS):
            prod[1, h, d] = value[:, h * part : (h + 1) * part].reshape(2, piece, part)

    everything = list(range(blocks))
    units = PARTS * turns
    settle_time = max(units, LEAD + turns * (PARTS - 1) + SKEW * turns + 1)
    end_time = LEAD + steps + SKEW * (turns - 1)
    relay_time = settle_time + 2
    relay_end = relay_time + PARTS

    def run(layer, some, begin, end, extra=None):
        def body(u, carry):
            send_step(layer, u - LEAD)
            if begin < units:
                @pl.when(u < units)
                def _():
                    h, i = u // turns, lax.rem(u, turns)
                    extra_unit = jnp.where(i == turns - 1, 1, 0)

                    def one(n, inner):
                        unit(layer, some, h, i + n)
                        return inner

                    lax.fori_loop(0, 1 + extra_unit, one, 0)

            if extra is not None:
                extra(u - begin)
            return carry

        lax.fori_loop(begin, end, body, 0)

    def hide(b):
        value = jnp.maximum(project(0, b), 0.0).astype(inputs.dtype)
        for h in range(PARTS):
            inputs[1, h, slot_rows(b, row), :] = value[:, h * part : (h + 1) * part]

    def gather_begin(layer, some):
        near_start(layer, some, 0)
        if PARTS > 1:
            near_start(layer, some, 1)

    def gather_next(layer, some):
        relay(layer, some, 0)
        if PARTS > 2:
            near_start(layer, some, 2)

    def early_relay(h):
        relay(1, [0], h)

        @pl.when(h + 2 < PARTS)
        def _():
            near_start(1, [0], h + 2)

    def drain(layer):
        for h in range(PARTS):
            for b in range(blocks):
                for i in range(len(bits)):
                    near_copy(layer, b, h, i).wait_send()
                for i in range(len(masks)):
                    for side in (0, 1):
                        far_copy(layer, b, h, i, side).wait_send()

            def drain_pair(d, carry):
                pair_copy(layer, h, d).wait_send()
                return carry

            lax.fori_loop(0, n_chip, drain_pair, 0)

        def drain_flow(k, carry):
            b, h, j = place_of(k)
            for way in (0, 1):
                d = turns - j if way == 0 else j
                ahead = d > chip if way == 0 else d < chip

                @pl.when(ahead)
                def _():
                    flow_copy(layer, way, k).wait_send()
                    if LINK_TYPES[layer] == jnp.int16:
                        scale_copy(way, k).wait_send()

            return carry

        lax.fori_loop(0, steps, drain_flow, 0)

    def out_copy(b):
        rows = pl.ds(b * sub, sub)
        return pltpu.make_async_copy(result.at[rows, :], out_hbm.at[rows, :], out_sem.at[b])

    for loads in feature_loads:
        for load in loads:
            load.wait()
    pl.semaphore_wait(barrier, peers)
    gather_begin(0, everything)

    tiles[slots] = jnp.zeros((tile, tile), tiles.dtype)
    spots = tile_rows * tile_cols
    counts_load.wait()
    places_load.wait()
    count = counts[row, col]
    order = lax.broadcasted_iota(jnp.int32, (spots, slots), 1)
    spot = lax.broadcasted_iota(jnp.int32, (spots, slots), 0)
    place = places[0:1, :] * tile_cols + places[1:2, :]
    listed = (place == spot) & (order < count)
    marks = jnp.where(listed, order - slots, 0)
    found = jnp.sum(marks.T, axis=0, keepdims=True) + slots
    inverse_rows[...] = jnp.broadcast_to(found, inverse_rows.shape)
    inverse_load = pltpu.make_async_copy(inverse_rows, inverse_ref, load_sem.at[3])
    inverse_load.start()
    inverse_load.wait()
    tile_load.wait()

    def place_row(i, carry):
        rows = pl.ds(pl.multiple_of(i * tile, tile), tile)
        for t in range(tile_cols):
            at = (t % blocks) * (tile_cols // blocks) + t // blocks
            slot = jnp.clip(inverse_ref[0, i * tile_cols + t], 0, slots)
            dense[rows, at * tile : (at + 1) * tile] = tiles[slot]
        return carry

    lax.fori_loop(0, tile_rows, place_row, 0)
    gather_next(0, everything)
    for load in weight_loads:
        load.wait()

    if blocks == 1:
        run(0, everything, 0, end_time)
    else:
        run(0, everything, 0, settle_time)
        settle(0, 0)
        hide(0)
        gather_begin(1, [0])
        run(0, everything, settle_time, relay_time)
        run(0, everything, relay_time, relay_end, early_relay)
        run(0, everything, relay_end, max(relay_end, end_time))
    settle(0, blocks - 1)
    hide(blocks - 1)
    late = [blocks - 1]
    gather_begin(1, late)
    if blocks > 1:
        for h in range(PARTS):
            arrive(1, [0], h)
        early_unit(0)
        early_unit(1)
        gather_next(1, late)
        for i in range(2, n_chip):
            early_unit(i)
    else:
        gather_next(1, late)
    if blocks == 1:
        run(1, late, 0, end_time)
    else:
        run(1, late, 0, settle_time)
        settle(1, 0)
        result[0:sub, :] = project(1, 0)
        out_copy(0).start()
        run(1, late, settle_time, end_time)
    drain(0)
    drain(1)
    settle(1, blocks - 1)
    result[(blocks - 1) * sub :, :] = project(1, blocks - 1)
    out_copy(blocks - 1).start()
    for b in range(blocks):
        out_copy(b).wait()


def shards(n_row, n_col, features, tile_values, tile_places, tile_counts, weight_one, weight_two):
    tiles = tile_values.reshape(tile_values.shape[2:])
    places = tile_places.reshape(tile_places.shape[2:])
    slots, tile = tiles.shape[0], tiles.shape[1]
    piece, width = features.shape
    part = width // PARTS
    blocks = 2 if piece == 2 * tile else 1
    sub = piece // blocks
    rows, depth = piece * n_col, piece * n_row
    tile_rows, tile_cols = rows // tile, depth // tile
    n_chip = n_col // 2
    spots = tile_rows * tile_cols
    steps = blocks * PARTS * (n_chip - 1)
    n_bits = (n_row - 1).bit_length()
    n_far = max(1, n_row - 1 - n_bits)

    def flow(layer):
        return pltpu.VMEM((steps, sub, part), LINK_TYPES[layer])

    dma = pltpu.SemaphoreType.DMA
    any_space = pl.BlockSpec(memory_space=pl.ANY)
    second = pl.pallas_call(
        functools.partial(kernel, n_row, n_col, blocks),
        out_shape=jax.ShapeDtypeStruct((piece, width), jnp.float32),
        in_specs=[any_space] * 6,
        out_specs=any_space,
        scratch_shapes=[
            pltpu.VMEM((slots + 1, tile, tile), jnp.bfloat16),
            pltpu.VMEM((rows, depth), jnp.bfloat16),
            pltpu.VMEM((2, width, width), jnp.float32),
            pltpu.VMEM((2, PARTS, depth, part), jnp.bfloat16),
            pltpu.VMEM((blocks, sub, width), jnp.float32),
            pltpu.VMEM((piece, width), jnp.float32),
            pltpu.VMEM((2, PARTS, n_chip, 2, piece, part), jnp.float32),
            pltpu.VMEM((2, PARTS, n_chip, piece, part), jnp.float32),
            flow(0), flow(0), flow(0), flow(0), flow(1), flow(1), flow(1), flow(1),
            pltpu.VMEM((2, steps, 1, part), jnp.float32),
            pltpu.VMEM((2, steps, 1, part), jnp.float32),
            dma((6,)), dma((blocks, PARTS)), dma((blocks,)),
            dma((2, blocks, PARTS, n_bits)), dma((2, blocks, PARTS, n_bits)),
            dma((2, blocks, PARTS, n_far, 2)), dma((2, blocks, PARTS, n_far, 2)),
            dma((2, PARTS, n_chip)), dma((2, PARTS, n_chip)),
            dma((2, 2, steps)), dma((2, 2, steps)),
            dma((2, steps)), dma((2, steps)),
            pltpu.SMEM(tile_counts.shape, jnp.int32), pltpu.VMEM(places.shape, jnp.int32),
            pltpu.VMEM((8, spots), jnp.int32), pltpu.SMEM((8, spots), jnp.int32),
        ],
        compiler_params=pltpu.CompilerParams(
            collective_id=0, has_side_effects=True, vmem_limit_bytes=60 * 1024 * 1024
        ),
    )(tile_counts, places, features, tiles, weight_one, weight_two)
    return jnp.maximum(second, 0.0)


def solution(mesh):
    placed = (
        P(("row", "col"), None),
        P("row", "col", None, None, None),
        P("row", "col", None, None),
        P(),
        P(),
        P(),
    )
    return jax.shard_map(
        functools.partial(shards, mesh.shape["row"], mesh.shape["col"]),
        mesh=mesh, in_specs=placed, out_specs=P(("row", "col"), None), check_vma=False,
    )
```

```python
import functools

import jax
import jax.numpy as jnp
from jax import lax
from jax.experimental import pallas as pl
from jax.experimental.pallas import tpu as pltpu
from jax.sharding import PartitionSpec as P

MESH = pl.DeviceIdType.MESH
PARTS = 4
LINK_TYPES = (jnp.int16, jnp.bfloat16)
TOP = 32766.0
LEAD = 2


def kernel(
    n_row, n_col, blocks,
    counts_hbm, places_hbm, features_hbm, tiles_hbm, weight_one_hbm, weight_two_hbm,
    out_hbm,
    tiles, dense, weights, inputs, total, result, prod, pair_in,
    out0, out1, land0, land1, via0, via1, scale_out, scale_land, scale_via,
    load_sem, feature_sem, out_sem, gather_send, gather_recv, pair_send, pair_recv,
    link_send, land_recv, via_recv, scale_send, scale_land_recv, scale_via_recv,
    counts, places, inverse_rows, inverse_ref,
):
    row, col = lax.axis_index("row"), lax.axis_index("col")
    n_chip = n_col // 2
    chip, core = col // 2, col % 2
    partner = chip * 2 + (1 - core)
    slots, tile = tiles_hbm.shape[0], tiles_hbm.shape[1]
    piece, width = features_hbm.shape
    part = width // PARTS
    sub = piece // blocks
    depth = piece * n_row
    tile_rows, tile_cols = dense.shape[0] // tile, depth // tile
    turns = n_chip - 1

    barrier = pltpu.get_barrier_semaphore()

    def greet(step, carry):
        pl.semaphore_signal(
            barrier, inc=1, device_id=(row, lax.rem(chip + step, n_chip) * 2 + core),
            device_id_type=MESH,
        )
        return carry

    lax.fori_loop(1, n_chip, greet, 0)
    for step in range(1, n_row):
        pl.semaphore_signal(
            barrier, inc=1, device_id=(lax.rem(row + step, n_row), col), device_id_type=MESH
        )
    pl.semaphore_signal(barrier, inc=1, device_id=(row, partner), device_id_type=MESH)

    def slot_rows(b, q):
        return pl.ds(pl.multiple_of((b * n_row + q) * sub, sub), sub)

    feature_loads = [
        [
            pltpu.make_async_copy(
                features_hbm.at[pl.ds(b * sub, sub), pl.ds(h * part, part)],
                inputs.at[0, h, slot_rows(b, row), :],
                feature_sem.at[b, h],
            )
            for b in range(blocks)
        ]
        for h in range(PARTS)
    ]
    for loads in feature_loads:
        for load in loads:
            load.start()
    peers = n_row - 1 + 1 + n_chip - 1
    end_chip = (chip == 0) | (chip == turns)
    neighbour = jnp.where(chip == 0, 1, turns - 1)

    def gather_copy(layer, b, h, step):
        block = inputs.at[layer, h, slot_rows(b, row), :]
        return pltpu.make_async_remote_copy(
            src_ref=block, dst_ref=block,
            send_sem=gather_send.at[layer, b, h, step - 1],
            recv_sem=gather_recv.at[layer, b, h, step - 1],
            device_id=(lax.rem(row + step, n_row), col), device_id_type=MESH,
        )

    def gather_start(layer, b, h):
        for step in range(1, n_row):
            gather_copy(layer, b, h, step).start()

    def gather_wait(layer, b, h):
        for step in range(1, n_row):
            gather_copy(layer, b, h, step).wait_recv()

    def pair_copy(layer, h, d):
        return pltpu.make_async_remote_copy(
            src_ref=prod.at[layer, h, d, 1 - core],
            dst_ref=pair_in.at[layer, h, d],
            send_sem=pair_send.at[layer, h, d], recv_sem=pair_recv.at[layer, h, d],
            device_id=(row, partner), device_id_type=MESH,
        )

    outs, lands, vias = (out0, out1), (land0, land1), (via0, via1)

    def spot_of(b, h, d):
        return (b * PARTS + h) * n_chip + d

    def link_copy(layer, b, h, d, target, scale, via):
        at, here = spot_of(b, h, d), spot_of(b, h, chip)
        if via:
            there = spot_of(b - 1, h, d)
            place = (scale_via if scale else vias[layer]).at[there]
            recv = (scale_via_recv if scale else via_recv.at[layer]).at[there]
        else:
            place = (scale_land if scale else lands[layer]).at[here]
            recv = (scale_land_recv if scale else land_recv.at[layer]).at[here]
        return pltpu.make_async_remote_copy(
            src_ref=(scale_out if scale else outs[layer]).at[at], dst_ref=place,
            send_sem=(scale_send if scale else link_send.at[layer]).at[at], recv_sem=recv,
            device_id=(row, target * 2 + core), device_id_type=MESH,
        )

    def both(layer):
        return (True, False) if LINK_TYPES[layer] == jnp.int16 else (False,)

    def post(layer, b, h, d, value):
        at = spot_of(b, h, d)
        if LINK_TYPES[layer] == jnp.int16:
            peak = jnp.maximum(jnp.max(jnp.abs(value), axis=0, keepdims=True), 1e-30)
            scale_out[at] = peak * (1.0 / TOP)
            outs[layer][at] = jnp.round(value * (TOP / peak)).astype(jnp.int32).astype(jnp.int16)
        else:
            outs[layer][at] = value.astype(outs[layer].dtype)
        if b == 0:
            for scale in both(layer):
                link_copy(layer, b, h, d, d, scale, False).start()
        else:
            detour = end_chip & (d != neighbour)

            @pl.when(detour)
            def _():
                for scale in both(layer):
                    link_copy(layer, b, h, d, neighbour, scale, True).start()

            @pl.when(jnp.logical_not(detour))
            def _():
                for scale in both(layer):
                    link_copy(layer, b, h, d, d, scale, False).start()

    def decode(layer, block, scale):
        if LINK_TYPES[layer] == jnp.int16:
            return block.astype(jnp.int32).astype(jnp.float32) * scale
        return block.astype(jnp.float32)

    def take_land(layer, b, h, s):
        at = spot_of(b, h, s)
        for scale in both(layer):
            pltpu.make_async_remote_copy(
                src_ref=(scale_out if scale else outs[layer]).at[at],
                dst_ref=(scale_land if scale else lands[layer]).at[at],
                send_sem=(scale_send if scale else link_send.at[layer]).at[at],
                recv_sem=(scale_land_recv if scale else land_recv.at[layer]).at[at],
                device_id=(row, partner), device_id_type=MESH,
            ).wait_recv()
        return decode(layer, lands[layer][at], scale_land[at])

    def take_via(layer, b, h, d):
        at = spot_of(b - 1, h, d)
        for scale in both(layer):
            link_copy(layer, b, h, d, partner // 2, scale, True).wait_recv()
        return decode(layer, vias[layer][at], scale_via[at])

    def pair_sum(layer, b, h, d):
        rows = pl.ds(b * sub, sub)
        return prod[layer, h, d, core, rows, :] + pair_in[layer, h, d, rows, :]

    def send(layer, b, h, d):
        if b == 0:
            post(layer, b, h, d, pair_sum(layer, b, h, d))
        else:
            merged = ((chip == 1) & (d > 1)) | ((chip == turns - 1) & (d < turns - 1))

            @pl.when(merged)
            def _():
                post(layer, b, h, d, pair_sum(layer, b, h, d) + take_via(layer, b, h, d))

            @pl.when(jnp.logical_not(merged))
            def _():
                post(layer, b, h, d, pair_sum(layer, b, h, d))

    def sources(b, s):
        if b == 0:
            return s != chip
        first_hop = ((s == 0) & (chip != 1)) | ((s == turns) & (chip != turns - 1))
        return (s != chip) & jnp.logical_not(first_hop)

    def settle(layer, b):
        for h in range(PARTS):
            columns = slice(h * part, (h + 1) * part)
            total[b, :, columns] = pair_sum(layer, b, h, chip)

            def add(s, carry):
                @pl.when(sources(b, s))
                def _():
                    total[b, :, columns] += take_land(layer, b, h, s)

                return carry

            lax.fori_loop(0, n_chip, add, 0)

    def project(layer, b):
        return jnp.dot(
            total[b], weights[layer], precision=lax.Precision.HIGHEST,
            preferred_element_type=jnp.float32,
        )

    def chip_rows(d):
        return pl.ds(pl.multiple_of(d * (2 * piece), 2 * piece), 2 * piece)

    def unit_chip(i):
        return jnp.where(chip < n_chip // 2, turns - i, i)

    def late_chip(i):
        return jnp.where(
            chip < n_chip // 2, lax.rem(n_chip - i, n_chip), lax.rem(turns + i, n_chip)
        )

    early = depth - depth // blocks
    known_parts = PARTS - 1

    def unit(layer, u):
        h, i = u // n_chip, lax.rem(u, n_chip)
        split = layer == 1 and blocks > 1

        @pl.when(i == 0)
        def _():
            if split:
                @pl.when(h >= known_parts)
                def _():
                    gather_wait(layer, 0, h)

                gather_wait(layer, 1, h)
            else:
                for b in range(blocks):
                    gather_wait(layer, b, h)

        d = unit_chip(i)

        def whole():
            value = jnp.dot(
                dense[chip_rows(d), :], inputs[layer, h], preferred_element_type=jnp.float32
            )
            prod[layer, h, d] = value.reshape(2, piece, part)

        if split:
            @pl.when(h < known_parts)
            def _():
                value = jnp.dot(
                    dense[chip_rows(d), early:], inputs[layer, h, early:, :],
                    preferred_element_type=jnp.float32,
                )
                prod[layer, h, d] += value.reshape(2, piece, part)

            @pl.when(h >= known_parts)
            def _():
                whole()
        else:
            whole()
        pair_copy(layer, h, d).start()

    def early_unit(i):
        d = unit_chip(i)
        known = jnp.concatenate([inputs[1, h, 0:early, :] for h in range(known_parts)], axis=1)
        value = jnp.dot(dense[chip_rows(d), 0:early], known, preferred_element_type=jnp.float32)
        for h in range(known_parts):
            prod[1, h, d] = value[:, h * part : (h + 1) * part].reshape(2, piece, part)

    units = PARTS * n_chip

    def run_first(layer):
        def body(u, carry):
            k = u - LEAD

            @pl.when(k >= 0)
            def _():
                h, d = k // n_chip, unit_chip(lax.rem(k, n_chip))
                pair_copy(layer, h, d).wait_recv()

                @pl.when(d != chip)
                def _():
                    send(layer, 0, h, d)

                @pl.when((d != chip) & end_chip & (h == 0))
                def _():
                    for b in range(1, blocks):
                        send(layer, b, h, d)

            @pl.when(u < units)
            def _():
                unit(layer, u)

            return carry

        lax.fori_loop(0, units + LEAD, body, 0)

    def run_rest(layer, begin, end):
        def body(w, carry):
            d, h = late_chip(w // PARTS), lax.rem(w, PARTS)

            @pl.when((d != chip) & jnp.logical_not(end_chip & (h == 0)))
            def _():
                for b in range(1, blocks):
                    send(layer, b, h, d)

            return carry

        if blocks > 1:
            lax.fori_loop(begin, end, body, 0)

    def hide(b):
        value = jnp.maximum(project(0, b), 0.0).astype(inputs.dtype)
        for h in range(PARTS):
            inputs[1, h, slot_rows(b, row), :] = value[:, h * part : (h + 1) * part]

    def drain(layer):
        for h in range(PARTS):
            for b in range(blocks):
                for step in range(1, n_row):
                    gather_copy(layer, b, h, step).wait_send()

        def drain_pair(d, carry):
            for h in range(PARTS):
                pair_copy(layer, h, d).wait_send()

                @pl.when(d != chip)
                def _():
                    for b in range(blocks):
                        for scale in both(layer):
                            link_copy(layer, b, h, d, d, scale, False).wait_send()

            return carry

        lax.fori_loop(0, n_chip, drain_pair, 0)

    def out_copy(b):
        rows = pl.ds(b * sub, sub)
        return pltpu.make_async_copy(result.at[rows, :], out_hbm.at[rows, :], out_sem.at[b])

    for loads in feature_loads:
        for load in loads:
            load.wait()
    counts_load = pltpu.make_async_copy(counts_hbm, counts, load_sem.at[4])
    counts_load.start()
    places_load = pltpu.make_async_copy(places_hbm, places, load_sem.at[5])
    places_load.start()
    tile_load = pltpu.make_async_copy(tiles_hbm, tiles.at[pl.ds(0, slots)], load_sem.at[0])
    tile_load.start()
    weight_loads = [
        pltpu.make_async_copy(weight_one_hbm, weights.at[0], load_sem.at[1]),
        pltpu.make_async_copy(weight_two_hbm, weights.at[1], load_sem.at[2]),
    ]
    for load in weight_loads:
        load.start()

    pl.semaphore_wait(barrier, peers)
    for h in range(PARTS):
        for b in range(blocks):
            gather_start(0, b, h)

    tiles[slots] = jnp.zeros((tile, tile), tiles.dtype)
    spots = tile_rows * tile_cols
    counts_load.wait()
    places_load.wait()
    count = counts[row, col]
    order = lax.broadcasted_iota(jnp.int32, (spots, slots), 1)
    spot = lax.broadcasted_iota(jnp.int32, (spots, slots), 0)
    place = places[0:1, :] * tile_cols + places[1:2, :]
    listed = (place == spot) & (order < count)
    marks = jnp.where(listed, order - slots, 0)
    found = jnp.sum(marks.T, axis=0, keepdims=True) + slots
    inverse_rows[...] = jnp.broadcast_to(found, inverse_rows.shape)
    inverse_load = pltpu.make_async_copy(inverse_rows, inverse_ref, load_sem.at[3])
    inverse_load.start()
    inverse_load.wait()
    tile_load.wait()

    def place_row(i, carry):
        rows = pl.ds(pl.multiple_of(i * tile, tile), tile)
        for t in range(tile_cols):
            at = (t % blocks) * (tile_cols // blocks) + t // blocks
            slot = jnp.clip(inverse_ref[0, i * tile_cols + t], 0, slots)
            dense[rows, at * tile : (at + 1) * tile] = tiles[slot]
        return carry

    lax.fori_loop(0, tile_rows, place_row, 0)
    for load in weight_loads:
        load.wait()

    middle = jnp.where(end_chip, units, units // 2)
    run_first(0)
    run_rest(0, 0, middle)
    if blocks > 1:
        settle(0, 0)
        hide(0)
        for h in range(known_parts):
            gather_start(1, 0, h)
    run_rest(0, middle, units)
    settle(0, blocks - 1)
    hide(blocks - 1)
    gather_start(1, blocks - 1, 0)
    if blocks > 1:
        for h in range(known_parts, PARTS):
            gather_start(1, 0, h)
    for h in range(1, PARTS):
        gather_start(1, blocks - 1, h)
    if blocks > 1:
        for h in range(known_parts):
            gather_wait(1, 0, h)
        for i in range(n_chip):
            early_unit(i)
    run_first(1)
    run_rest(1, 0, middle)
    drain(0)
    if blocks > 1:
        settle(1, 0)
        result[0:sub, :] = project(1, 0)
        out_copy(0).start()
    run_rest(1, middle, units)
    drain(1)
    settle(1, blocks - 1)
    result[(blocks - 1) * sub :, :] = project(1, blocks - 1)
    out_copy(blocks - 1).start()
    for b in range(blocks):
        out_copy(b).wait()


def shards(n_row, n_col, features, tile_values, tile_places, tile_counts, weight_one, weight_two):
    tiles = tile_values.reshape(tile_values.shape[2:])
    places = tile_places.reshape(tile_places.shape[2:])
    slots, tile = tiles.shape[0], tiles.shape[1]
    piece, width = features.shape
    part = width // PARTS
    blocks = 2 if piece == 2 * tile else 1
    sub = piece // blocks
    rows, depth = piece * n_col, piece * n_row
    tile_rows, tile_cols = rows // tile, depth // tile
    n_chip = n_col // 2
    spots = tile_rows * tile_cols
    items = blocks * PARTS * n_chip
    detours = max(1, (blocks - 1) * PARTS * n_chip)

    def flow(layer, count):
        return pltpu.VMEM((count, sub, part), LINK_TYPES[layer])

    def scales(count):
        return pltpu.VMEM((count, 1, part), jnp.float32)

    dma = pltpu.SemaphoreType.DMA
    any_space = pl.BlockSpec(memory_space=pl.ANY)
    second = pl.pallas_call(
        functools.partial(kernel, n_row, n_col, blocks),
        out_shape=jax.ShapeDtypeStruct((piece, width), jnp.float32),
        in_specs=[any_space] * 6,
        out_specs=any_space,
        scratch_shapes=[
            pltpu.VMEM((slots + 1, tile, tile), jnp.bfloat16),
            pltpu.VMEM((rows, depth), jnp.bfloat16),
            pltpu.VMEM((2, width, width), jnp.float32),
            pltpu.VMEM((2, PARTS, depth, part), jnp.bfloat16),
            pltpu.VMEM((blocks, sub, width), jnp.float32),
            pltpu.VMEM((piece, width), jnp.float32),
            pltpu.VMEM((2, PARTS, n_chip, 2, piece, part), jnp.float32),
            pltpu.VMEM((2, PARTS, n_chip, piece, part), jnp.float32),
            flow(0, items), flow(1, items), flow(0, items), flow(1, items),
            flow(0, detours), flow(1, detours),
            scales(items), scales(items), scales(detours),
            dma((6,)), dma((blocks, PARTS)), dma((blocks,)),
            dma((2, blocks, PARTS, n_row - 1)), dma((2, blocks, PARTS, n_row - 1)),
            dma((2, PARTS, n_chip)), dma((2, PARTS, n_chip)),
            dma((2, items)), dma((2, items)), dma((2, detours)),
            dma((items,)), dma((items,)), dma((detours,)),
            pltpu.SMEM(tile_counts.shape, jnp.int32), pltpu.VMEM(places.shape, jnp.int32),
            pltpu.VMEM((8, spots), jnp.int32), pltpu.SMEM((8, spots), jnp.int32),
        ],
        compiler_params=pltpu.CompilerParams(
            collective_id=0, has_side_effects=True, vmem_limit_bytes=60 * 1024 * 1024
        ),
    )(tile_counts, places, features, tiles, weight_one, weight_two)
    return jnp.maximum(second, 0.0)


def solution(mesh):
    placed = (
        P(("row", "col"), None),
        P("row", "col", None, None, None),
        P("row", "col", None, None),
        P(),
        P(),
        P(),
    )
    return jax.shard_map(
        functools.partial(shards, mesh.shape["row"], mesh.shape["col"]),
        mesh=mesh, in_specs=placed, out_specs=P(("row", "col"), None), check_vma=False,
    )
```

```python
import functools

import jax
import jax.numpy as jnp
from jax import lax
from jax.experimental import pallas as pl
from jax.experimental.pallas import tpu as pltpu
from jax.sharding import PartitionSpec as P

MESH = pl.DeviceIdType.MESH
PARTS = 4
LINK_TYPES = (jnp.int16, jnp.bfloat16)
TOP = 32766.0
LEAD = 3


def kernel(
    n_row, n_col, blocks,
    counts_hbm, places_hbm, features_hbm, tiles_hbm, weight_one_hbm, weight_two_hbm,
    out_hbm,
    tiles, dense, weights, inputs, total, result, prod, pair_in,
    out0, out1, land0, land1, via0, via1, scale_out, scale_land, scale_via,
    load_sem, feature_sem, out_sem, gather_send, gather_recv, pair_send, pair_recv,
    link_send, land_recv, via_recv, scale_send, scale_land_recv, scale_via_recv,
    counts, places, inverse_rows, inverse_ref,
):
    row, col = lax.axis_index("row"), lax.axis_index("col")
    n_chip = n_col // 2
    chip, core = col // 2, col % 2
    partner = chip * 2 + (1 - core)
    slots, tile = tiles_hbm.shape[0], tiles_hbm.shape[1]
    piece, width = features_hbm.shape
    part = width // PARTS
    sub = piece // blocks
    depth = piece * n_row
    tile_rows, tile_cols = dense.shape[0] // tile, depth // tile
    turns = n_chip - 1

    barrier = pltpu.get_barrier_semaphore()

    def greet(step, carry):
        pl.semaphore_signal(
            barrier, inc=1, device_id=(row, lax.rem(chip + step, n_chip) * 2 + core),
            device_id_type=MESH,
        )
        return carry

    lax.fori_loop(1, n_chip, greet, 0)
    for step in range(1, n_row):
        pl.semaphore_signal(
            barrier, inc=1, device_id=(lax.rem(row + step, n_row), col), device_id_type=MESH
        )
    pl.semaphore_signal(barrier, inc=1, device_id=(row, partner), device_id_type=MESH)

    def slot_rows(b, q):
        return pl.ds(pl.multiple_of((b * n_row + q) * sub, sub), sub)

    feature_loads = [
        [
            pltpu.make_async_copy(
                features_hbm.at[pl.ds(b * sub, sub), pl.ds(h * part, part)],
                inputs.at[0, h, slot_rows(b, row), :],
                feature_sem,
            )
            for b in range(blocks)
        ]
        for h in range(PARTS)
    ]
    for loads in feature_loads:
        for load in loads:
            load.start()
    peers = n_row - 1 + 1 + n_chip - 1
    end_chip = (chip == 0) | (chip == turns)
    neighbour = jnp.where(chip == 0, 1, turns - 1)

    def gather_copy(layer, b, h, step):
        block = inputs.at[layer, h, slot_rows(b, row), :]
        return pltpu.make_async_remote_copy(
            src_ref=block, dst_ref=block,
            send_sem=gather_send.at[layer], recv_sem=gather_recv.at[layer, b, h],
            device_id=(lax.rem(row + step, n_row), col), device_id_type=MESH,
        )

    def gather_start(layer, b, h):
        for step in range(1, n_row):
            gather_copy(layer, b, h, step).start()

    def whole_wait(block, send_sem, recv_sem):
        return pltpu.make_async_remote_copy(
            src_ref=block, dst_ref=block, send_sem=send_sem, recv_sem=recv_sem,
            device_id=(row, partner), device_id_type=MESH,
        )

    def gather_wait(layer, b, h):
        block = inputs.at[layer, h, pl.ds(0, (n_row - 1) * sub), :]
        whole_wait(block, gather_send.at[layer], gather_recv.at[layer, b, h]).wait_recv()

    def pair_copy(layer, h, d):
        return pltpu.make_async_remote_copy(
            src_ref=prod.at[layer, h, d, 1 - core],
            dst_ref=pair_in.at[layer, h, d],
            send_sem=pair_send.at[layer], recv_sem=pair_recv.at[layer, h, d],
            device_id=(row, partner), device_id_type=MESH,
        )

    outs, lands, vias = (out0, out1), (land0, land1), (via0, via1)

    def spot_of(b, h, d):
        return (b * PARTS + h) * n_chip + d

    def link_copy(layer, b, h, d, target, scale, via):
        at, here = spot_of(b, h, d), spot_of(b, h, chip)
        if via:
            there = spot_of(b - 1, h, d)
            place = (scale_via if scale else vias[layer]).at[there]
            recv = (scale_via_recv if scale else via_recv.at[layer]).at[there]
        else:
            place = (scale_land if scale else lands[layer]).at[here]
            recv = (scale_land_recv if scale else land_recv.at[layer]).at[b, chip]
        return pltpu.make_async_remote_copy(
            src_ref=(scale_out if scale else outs[layer]).at[at], dst_ref=place,
            send_sem=scale_send if scale else link_send.at[layer], recv_sem=recv,
            device_id=(row, target * 2 + core), device_id_type=MESH,
        )

    def both(layer):
        return (True, False) if LINK_TYPES[layer] == jnp.int16 else (False,)

    def post(layer, b, h, d, value):
        at = spot_of(b, h, d)
        if LINK_TYPES[layer] == jnp.int16:
            peak = jnp.maximum(jnp.max(jnp.abs(value), axis=0, keepdims=True), 1e-30)
            scale_out[at] = peak * (1.0 / TOP)
            outs[layer][at] = jnp.round(value * (TOP / peak)).astype(jnp.int32).astype(jnp.int16)
        else:
            outs[layer][at] = value.astype(outs[layer].dtype)
        if b == 0:
            for scale in both(layer):
                link_copy(layer, b, h, d, d, scale, False).start()
        else:
            detour = end_chip & (d != neighbour)

            @pl.when(detour)
            def _():
                for scale in both(layer):
                    link_copy(layer, b, h, d, neighbour, scale, True).start()

            @pl.when(jnp.logical_not(detour))
            def _():
                for scale in both(layer):
                    link_copy(layer, b, h, d, d, scale, False).start()

    def decode(layer, block, scale):
        if LINK_TYPES[layer] == jnp.int16:
            return block.astype(jnp.int32).astype(jnp.float32) * scale
        return block.astype(jnp.float32)

    def land_wait(layer, b, s):
        for scale in both(layer):
            whole_wait(
                (scale_land if scale else lands[layer]).at[pl.ds(0, PARTS)],
                scale_send if scale else link_send.at[layer],
                (scale_land_recv if scale else land_recv.at[layer]).at[b, s],
            ).wait_recv()

    def take_land(layer, b, h, s):
        at = spot_of(b, h, s)
        return decode(layer, lands[layer][at], scale_land[at])

    def take_via(layer, b, h, d):
        at = spot_of(b - 1, h, d)
        for scale in both(layer):
            link_copy(layer, b, h, d, partner // 2, scale, True).wait_recv()
        return decode(layer, vias[layer][at], scale_via[at])

    def pair_sum(layer, b, h, d):
        rows = pl.ds(b * sub, sub)
        return prod[layer, h, d, core, rows, :] + pair_in[layer, h, d, rows, :]

    def send(layer, b, h, d):
        if b == 0:
            post(layer, b, h, d, pair_sum(layer, b, h, d))
        else:
            merged = ((chip == 1) & (d > 1)) | ((chip == turns - 1) & (d < turns - 1))

            @pl.when(merged)
            def _():
                post(layer, b, h, d, pair_sum(layer, b, h, d) + take_via(layer, b, h, d))

            @pl.when(jnp.logical_not(merged))
            def _():
                post(layer, b, h, d, pair_sum(layer, b, h, d))

    def sources(b, s):
        if b == 0:
            return s != chip
        first_hop = ((s == 0) & (chip != 1)) | ((s == turns) & (chip != turns - 1))
        return (s != chip) & jnp.logical_not(first_hop)

    def settle(layer, b):
        for h in range(PARTS):
            total[b, :, h * part : (h + 1) * part] = pair_sum(layer, b, h, chip)

        def add(i, carry):
            s = late_chip(i)

            @pl.when(sources(b, s))
            def _():
                land_wait(layer, b, s)
                for h in range(PARTS):
                    total[b, :, h * part : (h + 1) * part] += take_land(layer, b, h, s)

            return carry

        lax.fori_loop(0, n_chip, add, 0)

    def project(layer, b):
        return jnp.dot(
            total[b], weights[layer], precision=lax.Precision.HIGHEST,
            preferred_element_type=jnp.float32,
        )

    def chip_rows(d):
        return pl.ds(pl.multiple_of(d * (2 * piece), 2 * piece), 2 * piece)

    def unit_chip(i):
        return jnp.where(chip < n_chip // 2, turns - i, i)

    def late_chip(i):
        return jnp.where(
            chip < n_chip // 2, lax.rem(n_chip - i, n_chip), lax.rem(turns + i, n_chip)
        )

    early = depth - depth // blocks
    known_parts = PARTS - 1

    def unit(layer, u):
        h, i = u // n_chip, lax.rem(u, n_chip)
        split = layer == 1 and blocks > 1

        @pl.when(i == 0)
        def _():
            if split:
                @pl.when(h >= known_parts)
                def _():
                    gather_wait(layer, 0, h)

                gather_wait(layer, 1, h)
            else:
                for b in range(blocks):
                    gather_wait(layer, b, h)

            @pl.when(h + 2 < PARTS)
            def _():
                if split:
                    @pl.when(h + 2 >= known_parts)
                    def _():
                        gather_start(layer, 0, h + 2)

                    gather_start(layer, 1, h + 2)
                else:
                    for b in range(blocks):
                        gather_start(layer, b, h + 2)

        d = unit_chip(i)

        def whole():
            value = jnp.dot(
                dense[chip_rows(d), :], inputs[layer, h], preferred_element_type=jnp.float32
            )
            prod[layer, h, d] = value.reshape(2, piece, part)

        if split:
            @pl.when(h < known_parts)
            def _():
                value = jnp.dot(
                    dense[chip_rows(d), early:], inputs[layer, h, early:, :],
                    preferred_element_type=jnp.float32,
                )
                prod[layer, h, d] += value.reshape(2, piece, part)

            @pl.when(h >= known_parts)
            def _():
                whole()
        else:
            whole()
        pair_copy(layer, h, d).start()

    def early_unit(i):
        d = unit_chip(i)
        known = jnp.concatenate([inputs[1, h, 0:early, :] for h in range(known_parts)], axis=1)
        value = jnp.dot(dense[chip_rows(d), 0:early], known, preferred_element_type=jnp.float32)
        for h in range(known_parts):
            prod[1, h, d] = value[:, h * part : (h + 1) * part].reshape(2, piece, part)

    units = PARTS * n_chip

    def run_first(layer):
        def body(u, carry):
            k = u - LEAD

            @pl.when(k >= 0)
            def _():
                h, d = k // n_chip, unit_chip(lax.rem(k, n_chip))
                pair_copy(layer, h, d).wait_recv()

                @pl.when(d != chip)
                def _():
                    send(layer, 0, h, d)

                @pl.when((d != chip) & end_chip & (h == 0))
                def _():
                    for b in range(1, blocks):
                        send(layer, b, h, d)

            @pl.when(u < units)
            def _():
                unit(layer, u)

            return carry

        lax.fori_loop(0, units + LEAD, body, 0)

    def run_rest(layer, begin, end):
        def body(w, carry):
            d, h = late_chip(w // PARTS), lax.rem(w, PARTS)

            @pl.when((d != chip) & jnp.logical_not(end_chip & (h == 0)))
            def _():
                for b in range(1, blocks):
                    send(layer, b, h, d)

            return carry

        if blocks > 1:
            lax.fori_loop(begin, end, body, 0)

    def hide(b):
        value = jnp.maximum(project(0, b), 0.0).astype(inputs.dtype)
        for h in range(PARTS):
            inputs[1, h, slot_rows(b, row), :] = value[:, h * part : (h + 1) * part]

    def drain(layer):
        sent = inputs.at[layer, :, pl.ds(0, depth // n_row * (n_row - 1)), :]
        whole_wait(sent, gather_send.at[layer], gather_recv.at[layer, 0, 0]).wait_send()
        whole_wait(
            pair_in.at[layer], pair_send.at[layer], pair_recv.at[layer, 0, 0]
        ).wait_send()
        for scale in both(layer):
            whole_wait(
                (scale_out if scale else outs[layer]).at[pl.ds(0, blocks * PARTS * turns)],
                scale_send if scale else link_send.at[layer],
                (scale_land_recv if scale else land_recv.at[layer]).at[0, 0],
            ).wait_send()

    def out_copy(b):
        rows = pl.ds(b * sub, sub)
        return pltpu.make_async_copy(result.at[rows, :], out_hbm.at[rows, :], out_sem.at[b])

    own = inputs.at[0, :, pl.ds(0, piece), :]
    pltpu.make_async_copy(own, own, feature_sem).wait()
    counts_load = pltpu.make_async_copy(counts_hbm, counts, load_sem.at[4])
    counts_load.start()
    places_load = pltpu.make_async_copy(places_hbm, places, load_sem.at[5])
    places_load.start()
    tile_load = pltpu.make_async_copy(tiles_hbm, tiles.at[pl.ds(0, slots)], load_sem.at[0])
    tile_load.start()
    weight_loads = [
        pltpu.make_async_copy(weight_one_hbm, weights.at[0], load_sem.at[1]),
        pltpu.make_async_copy(weight_two_hbm, weights.at[1], load_sem.at[2]),
    ]
    for load in weight_loads:
        load.start()

    pl.semaphore_wait(barrier, peers)
    for b in range(blocks):
        gather_start(0, b, 0)

    tiles[slots] = jnp.zeros((tile, tile), tiles.dtype)
    spots = tile_rows * tile_cols
    counts_load.wait()
    places_load.wait()
    count = counts[row, col]
    order = lax.broadcasted_iota(jnp.int32, (spots, slots), 1)
    spot = lax.broadcasted_iota(jnp.int32, (spots, slots), 0)
    place = places[0:1, :] * tile_cols + places[1:2, :]
    listed = (place == spot) & (order < count)
    marks = jnp.where(listed, order - slots, 0)
    found = jnp.sum(marks.T, axis=0, keepdims=True) + slots
    inverse_rows[...] = jnp.broadcast_to(found, inverse_rows.shape)
    inverse_load = pltpu.make_async_copy(inverse_rows, inverse_ref, load_sem.at[3])
    inverse_load.start()
    inverse_load.wait()
    tile_load.wait()

    def place_row(i, carry):
        rows = pl.ds(pl.multiple_of(i * tile, tile), tile)
        for t in range(tile_cols):
            at = (t % blocks) * (tile_cols // blocks) + t // blocks
            slot = jnp.clip(inverse_ref[0, i * tile_cols + t], 0, slots)
            dense[rows, at * tile : (at + 1) * tile] = tiles[slot]
        return carry

    lax.fori_loop(0, tile_rows, place_row, 0)
    for b in range(blocks):
        gather_start(0, b, 1)
    for load in weight_loads:
        load.wait()

    middle = jnp.where(end_chip, units, units // 2)
    run_first(0)
    run_rest(0, 0, middle)
    if blocks > 1:
        settle(0, 0)
        hide(0)
        for h in range(known_parts):
            gather_start(1, 0, h)
    run_rest(0, middle, units)
    settle(0, blocks - 1)
    hide(blocks - 1)
    gather_start(1, blocks - 1, 0)
    if blocks > 1:
        for h in range(known_parts):
            gather_wait(1, 0, h)
        for i in range(n_chip):
            early_unit(i)
    gather_start(1, blocks - 1, 1)
    run_first(1)
    run_rest(1, 0, middle)
    drain(0)
    if blocks > 1:
        settle(1, 0)
        result[0:sub, :] = project(1, 0)
        out_copy(0).start()
    run_rest(1, middle, units)
    drain(1)
    settle(1, blocks - 1)
    result[(blocks - 1) * sub :, :] = project(1, blocks - 1)
    out_copy(blocks - 1).start()
    for b in range(blocks):
        out_copy(b).wait()


def shards(n_row, n_col, features, tile_values, tile_places, tile_counts, weight_one, weight_two):
    tiles = tile_values.reshape(tile_values.shape[2:])
    places = tile_places.reshape(tile_places.shape[2:])
    slots, tile = tiles.shape[0], tiles.shape[1]
    piece, width = features.shape
    part = width // PARTS
    blocks = 2 if piece == 2 * tile else 1
    sub = piece // blocks
    rows, depth = piece * n_col, piece * n_row
    tile_rows, tile_cols = rows // tile, depth // tile
    n_chip = n_col // 2
    spots = tile_rows * tile_cols
    items = blocks * PARTS * n_chip
    detours = max(1, (blocks - 1) * PARTS * n_chip)

    def flow(layer, count):
        return pltpu.VMEM((count, sub, part), LINK_TYPES[layer])

    def scales(count):
        return pltpu.VMEM((count, 1, part), jnp.float32)

    dma = pltpu.SemaphoreType.DMA
    any_space = pl.BlockSpec(memory_space=pl.ANY)
    second = pl.pallas_call(
        functools.partial(kernel, n_row, n_col, blocks),
        out_shape=jax.ShapeDtypeStruct((piece, width), jnp.float32),
        in_specs=[any_space] * 6,
        out_specs=any_space,
        scratch_shapes=[
            pltpu.VMEM((slots + 1, tile, tile), jnp.bfloat16),
            pltpu.VMEM((rows, depth), jnp.bfloat16),
            pltpu.VMEM((2, width, width), jnp.float32),
            pltpu.VMEM((2, PARTS, depth, part), jnp.bfloat16),
            pltpu.VMEM((blocks, sub, width), jnp.float32),
            pltpu.VMEM((piece, width), jnp.float32),
            pltpu.VMEM((2, PARTS, n_chip, 2, piece, part), jnp.float32),
            pltpu.VMEM((2, PARTS, n_chip, piece, part), jnp.float32),
            flow(0, items), flow(1, items), flow(0, items), flow(1, items),
            flow(0, detours), flow(1, detours),
            scales(items), scales(items), scales(detours),
            dma((6,)), dma(()), dma((blocks,)),
            dma((2,)), dma((2, blocks, PARTS)),
            dma((2,)), dma((2, PARTS, n_chip)),
            dma((2,)), dma((2, blocks, n_chip)), dma((2, detours)),
            dma(()), dma((blocks, n_chip)), dma((detours,)),
            pltpu.SMEM(tile_counts.shape, jnp.int32), pltpu.VMEM(places.shape, jnp.int32),
            pltpu.VMEM((8, spots), jnp.int32), pltpu.SMEM((8, spots), jnp.int32),
        ],
        compiler_params=pltpu.CompilerParams(
            collective_id=0, has_side_effects=True, vmem_limit_bytes=60 * 1024 * 1024
        ),
    )(tile_counts, places, features, tiles, weight_one, weight_two)
    return jnp.maximum(second, 0.0)


def solution(mesh):
    placed = (
        P(("row", "col"), None),
        P("row", "col", None, None, None),
        P("row", "col", None, None),
        P(),
        P(),
        P(),
    )
    return jax.shard_map(
        functools.partial(shards, mesh.shape["row"], mesh.shape["col"]),
        mesh=mesh, in_specs=placed, out_specs=P(("row", "col"), None), check_vma=False,
    )
```

```python
import functools

import jax
import jax.numpy as jnp
from jax import lax
from jax.experimental import pallas as pl
from jax.experimental.pallas import tpu as pltpu
from jax.sharding import PartitionSpec as P

MESH = pl.DeviceIdType.MESH
PARTS = 4
LINK_TYPES = (jnp.int16, jnp.bfloat16)
TOP = 32766.0
LEAD = 3


def kernel(
    n_row, n_col, blocks,
    counts_hbm, places_hbm, features_hbm, tiles_hbm, weight_one_hbm, weight_two_hbm,
    out_ref,
    tiles, dense, weights, inputs, total, prod, pair_in,
    out0, out1, land0, land1, via0, via1, scale_out, scale_land, scale_via,
    load_sem, feature_sem, gather_send, gather_recv, pair_send, pair_recv,
    link_send, land_recv, via_recv, scale_send, scale_land_recv, scale_via_recv,
    counts, places, inverse_rows, inverse_ref,
):
    row, col = lax.axis_index("row"), lax.axis_index("col")
    n_chip = n_col // 2
    chip, core = col // 2, col % 2
    partner = chip * 2 + (1 - core)
    slots, tile = tiles_hbm.shape[0], tiles_hbm.shape[1]
    piece, width = features_hbm.shape
    part = width // PARTS
    sub = piece // blocks
    depth = piece * n_row
    tile_rows, tile_cols = dense.shape[0] // tile, depth // tile
    turns = n_chip - 1

    barrier = pltpu.get_barrier_semaphore()

    def greet(step, carry):
        pl.semaphore_signal(
            barrier, inc=1, device_id=(row, lax.rem(chip + step, n_chip) * 2 + core),
            device_id_type=MESH,
        )
        return carry

    lax.fori_loop(1, n_chip, greet, 0)
    for step in range(1, n_row):
        pl.semaphore_signal(
            barrier, inc=1, device_id=(lax.rem(row + step, n_row), col), device_id_type=MESH
        )
    pl.semaphore_signal(barrier, inc=1, device_id=(row, partner), device_id_type=MESH)

    def slot_rows(b, q):
        return pl.ds(pl.multiple_of((b * n_row + q) * sub, sub), sub)

    feature_loads = [
        [
            pltpu.make_async_copy(
                features_hbm.at[pl.ds(b * sub, sub), pl.ds(h * part, part)],
                inputs.at[0, h, slot_rows(b, row), :],
                feature_sem,
            )
            for b in range(blocks)
        ]
        for h in range(PARTS)
    ]
    for loads in feature_loads:
        for load in loads:
            load.start()
    peers = n_row - 1 + 1 + n_chip - 1
    end_chip = (chip == 0) | (chip == turns)
    neighbour = jnp.where(chip == 0, 1, turns - 1)

    def gather_copy(layer, b, h, step):
        block = inputs.at[layer, h, slot_rows(b, row), :]
        return pltpu.make_async_remote_copy(
            src_ref=block, dst_ref=block,
            send_sem=gather_send.at[layer], recv_sem=gather_recv.at[layer, b, h],
            device_id=(lax.rem(row + step, n_row), col), device_id_type=MESH,
        )

    def gather_start(layer, b, h):
        for step in range(1, n_row):
            gather_copy(layer, b, h, step).start()

    def whole_wait(block, send_sem, recv_sem):
        return pltpu.make_async_remote_copy(
            src_ref=block, dst_ref=block, send_sem=send_sem, recv_sem=recv_sem,
            device_id=(row, partner), device_id_type=MESH,
        )

    def gather_wait(layer, b, h):
        block = inputs.at[layer, h, pl.ds(0, (n_row - 1) * sub), :]
        whole_wait(block, gather_send.at[layer], gather_recv.at[layer, b, h]).wait_recv()

    def pair_copy(layer, h, d):
        return pltpu.make_async_remote_copy(
            src_ref=prod.at[layer, h, d, 1 - core],
            dst_ref=pair_in.at[layer, h, d],
            send_sem=pair_send.at[layer], recv_sem=pair_recv.at[layer, h, d],
            device_id=(row, partner), device_id_type=MESH,
        )

    outs, lands, vias = (out0, out1), (land0, land1), (via0, via1)

    def spot_of(b, h, d):
        return (b * PARTS + h) * n_chip + d

    def link_copy(layer, b, h, d, target, scale, via):
        at, here = spot_of(b, h, d), spot_of(b, h, chip)
        if via:
            there = spot_of(b - 1, h, d)
            place = (scale_via if scale else vias[layer]).at[there]
            recv = (scale_via_recv if scale else via_recv.at[layer]).at[there]
        else:
            place = (scale_land if scale else lands[layer]).at[here]
            recv = (scale_land_recv if scale else land_recv.at[layer]).at[b, chip]
        return pltpu.make_async_remote_copy(
            src_ref=(scale_out if scale else outs[layer]).at[at], dst_ref=place,
            send_sem=scale_send if scale else link_send.at[layer], recv_sem=recv,
            device_id=(row, target * 2 + core), device_id_type=MESH,
        )

    def both(layer):
        return (True, False) if LINK_TYPES[layer] == jnp.int16 else (False,)

    def post(layer, b, h, d, value):
        at = spot_of(b, h, d)
        if LINK_TYPES[layer] == jnp.int16:
            peak = jnp.maximum(jnp.max(jnp.abs(value), axis=0, keepdims=True), 1e-30)
            scale_out[at] = peak * (1.0 / TOP)
            outs[layer][at] = jnp.round(value * (TOP / peak)).astype(jnp.int32).astype(jnp.int16)
        else:
            outs[layer][at] = value.astype(outs[layer].dtype)
        if b == 0:
            for scale in both(layer):
                link_copy(layer, b, h, d, d, scale, False).start()
        else:
            detour = end_chip & (d != neighbour)

            @pl.when(detour)
            def _():
                for scale in both(layer):
                    link_copy(layer, b, h, d, neighbour, scale, True).start()

            @pl.when(jnp.logical_not(detour))
            def _():
                for scale in both(layer):
                    link_copy(layer, b, h, d, d, scale, False).start()

    def decode(layer, block, scale):
        if LINK_TYPES[layer] == jnp.int16:
            return block.astype(jnp.int32).astype(jnp.float32) * scale
        return block.astype(jnp.float32)

    def land_wait(layer, b, s):
        for scale in both(layer):
            whole_wait(
                (scale_land if scale else lands[layer]).at[pl.ds(0, PARTS)],
                scale_send if scale else link_send.at[layer],
                (scale_land_recv if scale else land_recv.at[layer]).at[b, s],
            ).wait_recv()

    def take_land(layer, b, h, s):
        at = spot_of(b, h, s)
        return decode(layer, lands[layer][at], scale_land[at])

    def take_via(layer, b, h, d):
        at = spot_of(b - 1, h, d)
        for scale in both(layer):
            link_copy(layer, b, h, d, partner // 2, scale, True).wait_recv()
        return decode(layer, vias[layer][at], scale_via[at])

    def pair_sum(layer, b, h, d):
        rows = pl.ds(b * sub, sub)
        return prod[layer, h, d, core, rows, :] + pair_in[layer, h, d, rows, :]

    def send(layer, b, h, d):
        if b == 0:
            post(layer, b, h, d, pair_sum(layer, b, h, d))
        else:
            merged = ((chip == 1) & (d > 1)) | ((chip == turns - 1) & (d < turns - 1))

            @pl.when(merged)
            def _():
                post(layer, b, h, d, pair_sum(layer, b, h, d) + take_via(layer, b, h, d))

            @pl.when(jnp.logical_not(merged))
            def _():
                post(layer, b, h, d, pair_sum(layer, b, h, d))

    def sources(b, s):
        if b == 0:
            return s != chip
        first_hop = ((s == 0) & (chip != 1)) | ((s == turns) & (chip != turns - 1))
        return (s != chip) & jnp.logical_not(first_hop)

    def settle(layer, b):
        for h in range(PARTS):
            total[b, :, h * part : (h + 1) * part] = pair_sum(layer, b, h, chip)

        def add(i, carry):
            s = late_chip(i)

            @pl.when(sources(b, s))
            def _():
                land_wait(layer, b, s)
                for h in range(PARTS):
                    total[b, :, h * part : (h + 1) * part] += take_land(layer, b, h, s)

            return carry

        lax.fori_loop(0, n_chip, add, 0)

    def project(layer, b):
        return jnp.dot(
            total[b], weights[layer], precision=lax.Precision.HIGHEST,
            preferred_element_type=jnp.float32,
        )

    def chip_rows(d):
        return pl.ds(pl.multiple_of(d * (2 * piece), 2 * piece), 2 * piece)

    def unit_chip(i):
        return jnp.where(chip < n_chip // 2, turns - i, i)

    def late_chip(i):
        return jnp.where(
            chip < n_chip // 2, lax.rem(n_chip - i, n_chip), lax.rem(turns + i, n_chip)
        )

    early = depth - depth // blocks
    known_parts = PARTS // 2

    def unit(layer, u):
        h, i = u // n_chip, lax.rem(u, n_chip)
        split = layer == 1 and blocks > 1

        @pl.when(i == 0)
        def _():
            if split:
                @pl.when(h >= known_parts)
                def _():
                    gather_wait(layer, 0, h)

                gather_wait(layer, 1, h)
            else:
                for b in range(blocks):
                    gather_wait(layer, b, h)

            @pl.when(h + 2 < PARTS)
            def _():
                if split:
                    @pl.when(h + 2 >= known_parts)
                    def _():
                        gather_start(layer, 0, h + 2)

                    gather_start(layer, 1, h + 2)
                else:
                    for b in range(blocks):
                        gather_start(layer, b, h + 2)

        d = unit_chip(i)

        def whole():
            value = jnp.dot(
                dense[chip_rows(d), :], inputs[layer, h], preferred_element_type=jnp.float32
            )
            prod[layer, h, d] = value.reshape(2, piece, part)

        if split:
            @pl.when(h < known_parts)
            def _():
                value = jnp.dot(
                    dense[chip_rows(d), early:], inputs[layer, h, early:, :],
                    preferred_element_type=jnp.float32,
                )
                prod[layer, h, d] += value.reshape(2, piece, part)

            @pl.when(h >= known_parts)
            def _():
                whole()
        else:
            whole()
        pair_copy(layer, h, d).start()

    def early_unit(i):
        d = unit_chip(i)
        known = jnp.concatenate([inputs[1, h, 0:early, :] for h in range(known_parts)], axis=1)
        value = jnp.dot(dense[chip_rows(d), 0:early], known, preferred_element_type=jnp.float32)
        for h in range(known_parts):
            prod[1, h, d] = value[:, h * part : (h + 1) * part].reshape(2, piece, part)

    units = PARTS * n_chip

    def run_first(layer):
        def body(u, carry):
            k = u - LEAD

            @pl.when(k >= 0)
            def _():
                h, d = k // n_chip, unit_chip(lax.rem(k, n_chip))
                pair_copy(layer, h, d).wait_recv()

                @pl.when(d != chip)
                def _():
                    send(layer, 0, h, d)

                @pl.when((d != chip) & end_chip & (h == 0))
                def _():
                    for b in range(1, blocks):
                        send(layer, b, h, d)

            @pl.when(u < units)
            def _():
                unit(layer, u)

            return carry

        lax.fori_loop(0, units + LEAD, body, 0)

    def run_merge(layer):
        def body(i, carry):
            d = late_chip(i)

            @pl.when((d != chip) & jnp.logical_not(end_chip))
            def _():
                for b in range(1, blocks):
                    send(layer, b, 0, d)

            return carry

        if blocks > 1:
            lax.fori_loop(1, n_chip, body, 0)

    def run_rest(layer, begin, end):
        def body(w, carry):
            d, h = late_chip(w // PARTS), lax.rem(w, PARTS)

            @pl.when((d != chip) & ((h > 0) | ((w == 0) & jnp.logical_not(end_chip))))
            def _():
                for b in range(1, blocks):
                    send(layer, b, h, d)

            return carry

        if blocks > 1:
            lax.fori_loop(begin, end, body, 0)

    def hide(b):
        value = jnp.maximum(project(0, b), 0.0).astype(inputs.dtype)
        for h in range(PARTS):
            inputs[1, h, slot_rows(b, row), :] = value[:, h * part : (h + 1) * part]

    def drain(layer):
        sent = inputs.at[layer, :, pl.ds(0, depth // n_row * (n_row - 1)), :]
        whole_wait(sent, gather_send.at[layer], gather_recv.at[layer, 0, 0]).wait_send()
        whole_wait(
            pair_in.at[layer], pair_send.at[layer], pair_recv.at[layer, 0, 0]
        ).wait_send()
        for scale in both(layer):
            whole_wait(
                (scale_out if scale else outs[layer]).at[pl.ds(0, blocks * PARTS * turns)],
                scale_send if scale else link_send.at[layer],
                (scale_land_recv if scale else land_recv.at[layer]).at[0, 0],
            ).wait_send()

    own = inputs.at[0, :, pl.ds(0, piece), :]
    pltpu.make_async_copy(own, own, feature_sem).wait()
    counts_load = pltpu.make_async_copy(counts_hbm, counts, load_sem.at[4])
    counts_load.start()
    places_load = pltpu.make_async_copy(places_hbm, places, load_sem.at[5])
    places_load.start()
    tile_load = pltpu.make_async_copy(tiles_hbm, tiles.at[pl.ds(0, slots)], load_sem.at[0])
    tile_load.start()
    weight_loads = [
        pltpu.make_async_copy(weight_one_hbm, weights.at[0], load_sem.at[1]),
        pltpu.make_async_copy(weight_two_hbm, weights.at[1], load_sem.at[2]),
    ]
    for load in weight_loads:
        load.start()

    pl.semaphore_wait(barrier, peers)
    for b in range(blocks):
        gather_start(0, b, 0)

    tiles[slots] = jnp.zeros((tile, tile), tiles.dtype)
    spots = tile_rows * tile_cols
    counts_load.wait()
    places_load.wait()
    count = counts[row, col]
    order = lax.broadcasted_iota(jnp.int32, (spots, slots), 1)
    spot = lax.broadcasted_iota(jnp.int32, (spots, slots), 0)
    place = places[0:1, :] * tile_cols + places[1:2, :]
    listed = (place == spot) & (order < count)
    marks = jnp.where(listed, order - slots, 0)
    found = jnp.sum(marks.T, axis=0, keepdims=True) + slots
    inverse_rows[...] = jnp.broadcast_to(found, inverse_rows.shape)
    inverse_load = pltpu.make_async_copy(inverse_rows, inverse_ref, load_sem.at[3])
    inverse_load.start()
    inverse_load.wait()
    tile_load.wait()

    def place_row(i, carry):
        rows = pl.ds(pl.multiple_of(i * tile, tile), tile)
        for t in range(tile_cols):
            at = (t % blocks) * (tile_cols // blocks) + t // blocks
            slot = jnp.clip(inverse_ref[0, i * tile_cols + t], 0, slots)
            dense[rows, at * tile : (at + 1) * tile] = tiles[slot]
        return carry

    lax.fori_loop(0, tile_rows, place_row, 0)
    for b in range(blocks):
        gather_start(0, b, 1)
    for load in weight_loads:
        load.wait()

    middle = jnp.where(end_chip, units, units // 2)
    run_first(0)
    run_merge(0)
    run_rest(0, 0, middle)
    if blocks > 1:
        settle(0, 0)
        hide(0)
        for h in range(known_parts):
            gather_start(1, 0, h)
    run_rest(0, middle, units)
    settle(0, blocks - 1)
    hide(blocks - 1)
    gather_start(1, blocks - 1, 0)
    if blocks > 1:
        for h in range(known_parts):
            gather_wait(1, 0, h)
        for i in range(n_chip):
            early_unit(i)
    gather_start(1, blocks - 1, 1)
    run_first(1)
    run_merge(1)
    run_rest(1, 0, middle)
    drain(0)
    if blocks > 1:
        settle(1, 0)
        out_ref[0:sub, :] = project(1, 0)
    run_rest(1, middle, units)
    drain(1)
    settle(1, blocks - 1)
    out_ref[(blocks - 1) * sub :, :] = project(1, blocks - 1)


def shards(n_row, n_col, features, tile_values, tile_places, tile_counts, weight_one, weight_two):
    tiles = tile_values.reshape(tile_values.shape[2:])
    places = tile_places.reshape(tile_places.shape[2:])
    slots, tile = tiles.shape[0], tiles.shape[1]
    piece, width = features.shape
    part = width // PARTS
    blocks = 2 if piece == 2 * tile else 1
    sub = piece // blocks
    rows, depth = piece * n_col, piece * n_row
    tile_rows, tile_cols = rows // tile, depth // tile
    n_chip = n_col // 2
    spots = tile_rows * tile_cols
    items = blocks * PARTS * n_chip
    detours = max(1, (blocks - 1) * PARTS * n_chip)

    def flow(layer, count):
        return pltpu.VMEM((count, sub, part), LINK_TYPES[layer])

    def scales(count):
        return pltpu.VMEM((count, 1, part), jnp.float32)

    dma = pltpu.SemaphoreType.DMA
    hbm = pl.BlockSpec(memory_space=pltpu.HBM)
    second = pl.pallas_call(
        functools.partial(kernel, n_row, n_col, blocks),
        out_shape=jax.ShapeDtypeStruct((piece, width), jnp.float32),
        in_specs=[hbm] * 6,
        out_specs=pl.BlockSpec(memory_space=pltpu.VMEM),
        scratch_shapes=[
            pltpu.VMEM((slots + 1, tile, tile), jnp.bfloat16),
            pltpu.VMEM((rows, depth), jnp.bfloat16),
            pltpu.VMEM((2, width, width), jnp.float32),
            pltpu.VMEM((2, PARTS, depth, part), jnp.bfloat16),
            pltpu.VMEM((blocks, sub, width), jnp.float32),
            pltpu.VMEM((2, PARTS, n_chip, 2, piece, part), jnp.float32),
            pltpu.VMEM((2, PARTS, n_chip, piece, part), jnp.float32),
            flow(0, items), flow(1, items), flow(0, items), flow(1, items),
            flow(0, detours), flow(1, detours),
            scales(items), scales(items), scales(detours),
            dma((6,)), dma(()),
            dma((2,)), dma((2, blocks, PARTS)),
            dma((2,)), dma((2, PARTS, n_chip)),
            dma((2,)), dma((2, blocks, n_chip)), dma((2, detours)),
            dma(()), dma((blocks, n_chip)), dma((detours,)),
            pltpu.SMEM(tile_counts.shape, jnp.int32), pltpu.VMEM(places.shape, jnp.int32),
            pltpu.VMEM((8, spots), jnp.int32), pltpu.SMEM((8, spots), jnp.int32),
        ],
        compiler_params=pltpu.CompilerParams(
            collective_id=0, has_side_effects=True, vmem_limit_bytes=40 * 1024 * 1024
        ),
    )(*(
        pltpu.with_memory_space_constraint(x, pltpu.HBM)
        for x in (tile_counts, places, features, tiles, weight_one, weight_two)
    ))
    return jnp.maximum(second, 0.0)


def solution(mesh):
    placed = (
        P(("row", "col"), None),
        P("row", "col", None, None, None),
        P("row", "col", None, None),
        P(),
        P(),
        P(),
    )
    return jax.shard_map(
        functools.partial(shards, mesh.shape["row"], mesh.shape["col"]),
        mesh=mesh, in_specs=placed, out_specs=P(("row", "col"), None), check_vma=False,
    )
```

```python
import functools

import jax
import jax.numpy as jnp
from jax import lax
from jax.experimental import pallas as pl
from jax.experimental.pallas import tpu as pltpu
from jax.sharding import PartitionSpec as P

MESH = pl.DeviceIdType.MESH
PARTS = 4
LINK_TYPES = (jnp.int16, jnp.bfloat16)
TOP = 32766.0
LEAD = 3


def kernel(
    n_row, n_col, blocks,
    counts_hbm, places_hbm, features_hbm, tiles_hbm, weight_one_hbm, weight_two_hbm,
    out_ref,
    tiles, dense, weights, inputs, total, prod, pair_in,
    out0, out1, land0, land1, via0, via1, scale_out, scale_land, scale_via,
    wave, load_sem, feature_sem, gather_send, gather_recv, pair_send, pair_recv,
    link_send, land_recv, via_recv, scale_send, scale_land_recv, scale_via_recv,
    counts, places, inverse_rows, inverse_ref,
):
    row, col = lax.axis_index("row"), lax.axis_index("col")
    n_chip = n_col // 2
    chip, core = col // 2, col % 2
    partner = chip * 2 + (1 - core)
    slots, tile = tiles_hbm.shape[0], tiles_hbm.shape[1]
    piece, width = features_hbm.shape
    part = width // PARTS
    sub = piece // blocks
    depth = piece * n_row
    tile_rows, tile_cols = dense.shape[0] // tile, depth // tile
    turns = n_chip - 1

    barrier = pltpu.get_barrier_semaphore()

    def beside(way):
        return (row, (chip + way) * 2 + core)

    @pl.when(chip > 0)
    def _():
        pl.semaphore_signal(barrier, inc=1, device_id=beside(-1), device_id_type=MESH)

    @pl.when(chip < n_chip - 1)
    def _():
        pl.semaphore_signal(barrier, inc=1, device_id=beside(1), device_id_type=MESH)

    for step in range(1, n_row):
        pl.semaphore_signal(
            barrier, inc=1, device_id=(lax.rem(row + step, n_row), col), device_id_type=MESH
        )
    pl.semaphore_signal(barrier, inc=1, device_id=(row, partner), device_id_type=MESH)

    def slot_rows(b, q):
        return pl.ds(pl.multiple_of((b * n_row + q) * sub, sub), sub)

    feature_loads = [
        [
            pltpu.make_async_copy(
                features_hbm.at[pl.ds(b * sub, sub), pl.ds(h * part, part)],
                inputs.at[0, h, slot_rows(b, row), :],
                feature_sem,
            )
            for b in range(blocks)
        ]
        for h in range(PARTS)
    ]
    for loads in feature_loads:
        for load in loads:
            load.start()
    peers = n_row + jnp.where(chip > 0, 1, 0) + jnp.where(chip < n_chip - 1, 1, 0)
    lower = chip < n_chip // 2
    end_chip = (chip == 0) | (chip == turns)
    neighbour = jnp.where(chip == 0, 1, turns - 1)

    def gather_copy(layer, b, h, step):
        block = inputs.at[layer, h, slot_rows(b, row), :]
        return pltpu.make_async_remote_copy(
            src_ref=block, dst_ref=block,
            send_sem=gather_send.at[layer], recv_sem=gather_recv.at[layer, b, h],
            device_id=(lax.rem(row + step, n_row), col), device_id_type=MESH,
        )

    def gather_start(layer, b, h):
        for step in range(1, n_row):
            gather_copy(layer, b, h, step).start()

    def whole_wait(block, send_sem, recv_sem):
        return pltpu.make_async_remote_copy(
            src_ref=block, dst_ref=block, send_sem=send_sem, recv_sem=recv_sem,
            device_id=(row, partner), device_id_type=MESH,
        )

    def gather_wait(layer, b, h):
        block = inputs.at[layer, h, pl.ds(0, (n_row - 1) * sub), :]
        whole_wait(block, gather_send.at[layer], gather_recv.at[layer, b, h]).wait_recv()

    def pass_on(way, waits):
        at = 0 if way > 0 else 1
        if waits:
            pl.semaphore_wait(wave.at[at], 1)

        @pl.when((chip < n_chip - 1) if way > 0 else (chip > 0))
        def _():
            pl.semaphore_signal(wave.at[at], inc=1, device_id=beside(way), device_id_type=MESH)

    def pair_copy(layer, h, d):
        return pltpu.make_async_remote_copy(
            src_ref=prod.at[layer, h, d, 1 - core],
            dst_ref=pair_in.at[layer, h, d],
            send_sem=pair_send.at[layer], recv_sem=pair_recv.at[layer, h, d],
            device_id=(row, partner), device_id_type=MESH,
        )

    outs, lands, vias = (out0, out1), (land0, land1), (via0, via1)

    def spot_of(b, h, d):
        return (b * PARTS + h) * n_chip + d

    def link_copy(layer, b, h, d, target, scale, via):
        at, here = spot_of(b, h, d), spot_of(b, h, chip)
        if via:
            there = spot_of(b - 1, h, d)
            place = (scale_via if scale else vias[layer]).at[there]
            recv = (scale_via_recv if scale else via_recv.at[layer]).at[there]
        else:
            place = (scale_land if scale else lands[layer]).at[here]
            recv = (scale_land_recv if scale else land_recv.at[layer]).at[b, chip]
        return pltpu.make_async_remote_copy(
            src_ref=(scale_out if scale else outs[layer]).at[at], dst_ref=place,
            send_sem=scale_send if scale else link_send.at[layer], recv_sem=recv,
            device_id=(row, target * 2 + core), device_id_type=MESH,
        )

    def both(layer):
        return (True, False) if LINK_TYPES[layer] == jnp.int16 else (False,)

    def post(layer, b, h, d, value):
        at = spot_of(b, h, d)
        if LINK_TYPES[layer] == jnp.int16:
            peak = jnp.maximum(jnp.max(jnp.abs(value), axis=0, keepdims=True), 1e-30)
            scale_out[at] = peak * (1.0 / TOP)
            outs[layer][at] = jnp.round(value * (TOP / peak)).astype(jnp.int32).astype(jnp.int16)
        else:
            outs[layer][at] = value.astype(outs[layer].dtype)
        if b == 0:
            for scale in both(layer):
                link_copy(layer, b, h, d, d, scale, False).start()
        else:
            detour = end_chip & (d != neighbour)

            @pl.when(detour)
            def _():
                for scale in both(layer):
                    link_copy(layer, b, h, d, neighbour, scale, True).start()

            @pl.when(jnp.logical_not(detour))
            def _():
                for scale in both(layer):
                    link_copy(layer, b, h, d, d, scale, False).start()

    def decode(layer, block, scale):
        if LINK_TYPES[layer] == jnp.int16:
            return block.astype(jnp.int32).astype(jnp.float32) * scale
        return block.astype(jnp.float32)

    def land_wait(layer, b, s):
        for scale in both(layer):
            whole_wait(
                (scale_land if scale else lands[layer]).at[pl.ds(0, PARTS)],
                scale_send if scale else link_send.at[layer],
                (scale_land_recv if scale else land_recv.at[layer]).at[b, s],
            ).wait_recv()

    def take_land(layer, b, h, s):
        at = spot_of(b, h, s)
        return decode(layer, lands[layer][at], scale_land[at])

    def take_via(layer, b, h, d):
        at = spot_of(b - 1, h, d)
        for scale in both(layer):
            link_copy(layer, b, h, d, partner // 2, scale, True).wait_recv()
        return decode(layer, vias[layer][at], scale_via[at])

    def pair_sum(layer, b, h, d):
        rows = pl.ds(b * sub, sub)
        return prod[layer, h, d, core, rows, :] + pair_in[layer, h, d, rows, :]

    def send(layer, b, h, d):
        if b == 0:
            post(layer, b, h, d, pair_sum(layer, b, h, d))
        else:
            merged = ((chip == 1) & (d > 1)) | ((chip == turns - 1) & (d < turns - 1))

            @pl.when(merged)
            def _():
                post(layer, b, h, d, pair_sum(layer, b, h, d) + take_via(layer, b, h, d))

            @pl.when(jnp.logical_not(merged))
            def _():
                post(layer, b, h, d, pair_sum(layer, b, h, d))

    def sources(b, s):
        if b == 0:
            return s != chip
        first_hop = ((s == 0) & (chip != 1)) | ((s == turns) & (chip != turns - 1))
        return (s != chip) & jnp.logical_not(first_hop)

    def settle(layer, b):
        for h in range(PARTS):
            total[b, :, h * part : (h + 1) * part] = pair_sum(layer, b, h, chip)

        def add(i, carry):
            s = late_chip(i)

            @pl.when(sources(b, s))
            def _():
                land_wait(layer, b, s)
                for h in range(PARTS):
                    total[b, :, h * part : (h + 1) * part] += take_land(layer, b, h, s)

            return carry

        lax.fori_loop(0, n_chip, add, 0)

    def project(layer, b):
        return jnp.dot(
            total[b], weights[layer], precision=lax.Precision.HIGHEST,
            preferred_element_type=jnp.float32,
        )

    def chip_rows(d):
        return pl.ds(pl.multiple_of(d * (2 * piece), 2 * piece), 2 * piece)

    def unit_chip(i):
        return jnp.where(chip < n_chip // 2, turns - i, i)

    def late_chip(i):
        return jnp.where(
            chip < n_chip // 2, lax.rem(n_chip - i, n_chip), lax.rem(turns + i, n_chip)
        )

    early = depth - depth // blocks
    known_parts = PARTS // 2

    def unit(layer, u):
        h, i = u // n_chip, lax.rem(u, n_chip)
        split = layer == 1 and blocks > 1

        @pl.when(i == 0)
        def _():
            if split:
                @pl.when(h >= known_parts)
                def _():
                    gather_wait(layer, 0, h)

                gather_wait(layer, 1, h)
            else:
                for b in range(blocks):
                    gather_wait(layer, b, h)

            @pl.when(h + 2 < PARTS)
            def _():
                if split:
                    @pl.when(h + 2 >= known_parts)
                    def _():
                        gather_start(layer, 0, h + 2)

                    gather_start(layer, 1, h + 2)
                else:
                    for b in range(blocks):
                        gather_start(layer, b, h + 2)

        d = unit_chip(i)

        def whole():
            value = jnp.dot(
                dense[chip_rows(d), :], inputs[layer, h], preferred_element_type=jnp.float32
            )
            prod[layer, h, d] = value.reshape(2, piece, part)

        if split:
            @pl.when(h < known_parts)
            def _():
                value = jnp.dot(
                    dense[chip_rows(d), early:], inputs[layer, h, early:, :],
                    preferred_element_type=jnp.float32,
                )
                prod[layer, h, d] += value.reshape(2, piece, part)

            @pl.when(h >= known_parts)
            def _():
                whole()
        else:
            whole()
        pair_copy(layer, h, d).start()

    def early_unit(i):
        d = unit_chip(i)
        known = jnp.concatenate([inputs[1, h, 0:early, :] for h in range(known_parts)], axis=1)
        value = jnp.dot(dense[chip_rows(d), 0:early], known, preferred_element_type=jnp.float32)
        for h in range(known_parts):
            prod[1, h, d] = value[:, h * part : (h + 1) * part].reshape(2, piece, part)

    units = PARTS * n_chip

    def run_first(layer):
        def body(u, carry):
            k = u - LEAD

            @pl.when(k >= 0)
            def _():
                h, d = k // n_chip, unit_chip(lax.rem(k, n_chip))
                pair_copy(layer, h, d).wait_recv()

                @pl.when(d != chip)
                def _():
                    send(layer, 0, h, d)

                @pl.when((d != chip) & end_chip & (h == 0))
                def _():
                    for b in range(1, blocks):
                        send(layer, b, h, d)

            @pl.when(u < units)
            def _():
                unit(layer, u)

            return carry

        lax.fori_loop(0, units + LEAD, body, 0)

    def run_merge(layer):
        def body(i, carry):
            d = late_chip(i)

            @pl.when((d != chip) & jnp.logical_not(end_chip))
            def _():
                for b in range(1, blocks):
                    send(layer, b, 0, d)

            return carry

        if blocks > 1:
            lax.fori_loop(1, n_chip, body, 0)

    def run_rest(layer, begin, end):
        def body(w, carry):
            d, h = late_chip(w // PARTS), lax.rem(w, PARTS)

            @pl.when((d != chip) & ((h > 0) | ((w == 0) & jnp.logical_not(end_chip))))
            def _():
                for b in range(1, blocks):
                    send(layer, b, h, d)

            return carry

        if blocks > 1:
            lax.fori_loop(begin, end, body, 0)

    def hide(b):
        value = jnp.maximum(project(0, b), 0.0).astype(inputs.dtype)
        for h in range(PARTS):
            inputs[1, h, slot_rows(b, row), :] = value[:, h * part : (h + 1) * part]

    def drain(layer):
        sent = inputs.at[layer, :, pl.ds(0, depth // n_row * (n_row - 1)), :]
        whole_wait(sent, gather_send.at[layer], gather_recv.at[layer, 0, 0]).wait_send()
        whole_wait(
            pair_in.at[layer], pair_send.at[layer], pair_recv.at[layer, 0, 0]
        ).wait_send()
        for scale in both(layer):
            whole_wait(
                (scale_out if scale else outs[layer]).at[pl.ds(0, blocks * PARTS * turns)],
                scale_send if scale else link_send.at[layer],
                (scale_land_recv if scale else land_recv.at[layer]).at[0, 0],
            ).wait_send()

    own = inputs.at[0, :, pl.ds(0, piece), :]
    pltpu.make_async_copy(own, own, feature_sem).wait()
    counts_load = pltpu.make_async_copy(counts_hbm, counts, load_sem.at[4])
    counts_load.start()
    places_load = pltpu.make_async_copy(places_hbm, places, load_sem.at[5])
    places_load.start()
    tile_load = pltpu.make_async_copy(tiles_hbm, tiles.at[pl.ds(0, slots)], load_sem.at[0])
    tile_load.start()
    weight_loads = [
        pltpu.make_async_copy(weight_one_hbm, weights.at[0], load_sem.at[1]),
        pltpu.make_async_copy(weight_two_hbm, weights.at[1], load_sem.at[2]),
    ]
    for load in weight_loads:
        load.start()

    pl.semaphore_wait(barrier, peers)
    for b in range(blocks):
        gather_start(0, b, 0)

    @pl.when(chip == 0)
    def _():
        pass_on(1, False)

    @pl.when(chip == n_chip - 1)
    def _():
        pass_on(-1, False)

    tiles[slots] = jnp.zeros((tile, tile), tiles.dtype)
    spots = tile_rows * tile_cols
    counts_load.wait()
    places_load.wait()
    count = counts[row, col]
    order = lax.broadcasted_iota(jnp.int32, (spots, slots), 1)
    spot = lax.broadcasted_iota(jnp.int32, (spots, slots), 0)
    place = places[0:1, :] * tile_cols + places[1:2, :]
    listed = (place == spot) & (order < count)
    marks = jnp.where(listed, order - slots, 0)
    found = jnp.sum(marks.T, axis=0, keepdims=True) + slots
    inverse_rows[...] = jnp.broadcast_to(found, inverse_rows.shape)
    inverse_load = pltpu.make_async_copy(inverse_rows, inverse_ref, load_sem.at[3])
    inverse_load.start()
    inverse_load.wait()

    @pl.when(lower & (chip > 0))
    def _():
        pass_on(1, True)

    @pl.when(jnp.logical_not(lower) & (chip < n_chip - 1))
    def _():
        pass_on(-1, True)

    tile_load.wait()

    def place_row(i, carry):
        rows = pl.ds(pl.multiple_of(i * tile, tile), tile)
        for t in range(tile_cols):
            at = (t % blocks) * (tile_cols // blocks) + t // blocks
            slot = jnp.clip(inverse_ref[0, i * tile_cols + t], 0, slots)
            dense[rows, at * tile : (at + 1) * tile] = tiles[slot]
        return carry

    lax.fori_loop(0, tile_rows, place_row, 0)
    for b in range(blocks):
        gather_start(0, b, 1)

    @pl.when(lower)
    def _():
        pass_on(-1, True)

    @pl.when(jnp.logical_not(lower))
    def _():
        pass_on(1, True)

    for load in weight_loads:
        load.wait()

    middle = jnp.where(end_chip, units, units // 2)
    run_first(0)
    run_merge(0)
    run_rest(0, 0, middle)
    if blocks > 1:
        settle(0, 0)
        hide(0)
        for h in range(known_parts):
            gather_start(1, 0, h)
    run_rest(0, middle, units)
    settle(0, blocks - 1)
    hide(blocks - 1)
    gather_start(1, blocks - 1, 0)
    if blocks > 1:
        for h in range(known_parts):
            gather_wait(1, 0, h)
        for i in range(n_chip):
            early_unit(i)
    gather_start(1, blocks - 1, 1)
    run_first(1)
    run_merge(1)
    run_rest(1, 0, middle)
    drain(0)
    if blocks > 1:
        settle(1, 0)
        out_ref[0:sub, :] = project(1, 0)
    run_rest(1, middle, units)
    drain(1)
    settle(1, blocks - 1)
    out_ref[(blocks - 1) * sub :, :] = project(1, blocks - 1)


def shards(n_row, n_col, features, tile_values, tile_places, tile_counts, weight_one, weight_two):
    tiles = tile_values.reshape(tile_values.shape[2:])
    places = tile_places.reshape(tile_places.shape[2:])
    slots, tile = tiles.shape[0], tiles.shape[1]
    piece, width = features.shape
    part = width // PARTS
    blocks = 2 if piece == 2 * tile else 1
    sub = piece // blocks
    rows, depth = piece * n_col, piece * n_row
    tile_rows, tile_cols = rows // tile, depth // tile
    n_chip = n_col // 2
    spots = tile_rows * tile_cols
    items = blocks * PARTS * n_chip
    detours = max(1, (blocks - 1) * PARTS * n_chip)

    def flow(layer, count):
        return pltpu.VMEM((count, sub, part), LINK_TYPES[layer])

    def scales(count):
        return pltpu.VMEM((count, 1, part), jnp.float32)

    dma = pltpu.SemaphoreType.DMA
    hbm = pl.BlockSpec(memory_space=pltpu.HBM)
    second = pl.pallas_call(
        functools.partial(kernel, n_row, n_col, blocks),
        out_shape=jax.ShapeDtypeStruct((piece, width), jnp.float32),
        in_specs=[hbm] * 6,
        out_specs=pl.BlockSpec(memory_space=pltpu.VMEM),
        scratch_shapes=[
            pltpu.VMEM((slots + 1, tile, tile), jnp.bfloat16),
            pltpu.VMEM((rows, depth), jnp.bfloat16),
            pltpu.VMEM((2, width, width), jnp.float32),
            pltpu.VMEM((2, PARTS, depth, part), jnp.bfloat16),
            pltpu.VMEM((blocks, sub, width), jnp.float32),
            pltpu.VMEM((2, PARTS, n_chip, 2, piece, part), jnp.float32),
            pltpu.VMEM((2, PARTS, n_chip, piece, part), jnp.float32),
            flow(0, items), flow(1, items), flow(0, items), flow(1, items),
            flow(0, detours), flow(1, detours),
            scales(items), scales(items), scales(detours),
            pltpu.SemaphoreType.REGULAR((2,)), dma((6,)), dma(()),
            dma((2,)), dma((2, blocks, PARTS)),
            dma((2,)), dma((2, PARTS, n_chip)),
            dma((2,)), dma((2, blocks, n_chip)), dma((2, detours)),
            dma(()), dma((blocks, n_chip)), dma((detours,)),
            pltpu.SMEM(tile_counts.shape, jnp.int32), pltpu.VMEM(places.shape, jnp.int32),
            pltpu.VMEM((8, spots), jnp.int32), pltpu.SMEM((8, spots), jnp.int32),
        ],
        compiler_params=pltpu.CompilerParams(
            collective_id=0, has_side_effects=True, vmem_limit_bytes=40 * 1024 * 1024
        ),
    )(*(
        pltpu.with_memory_space_constraint(x, pltpu.HBM)
        for x in (tile_counts, places, features, tiles, weight_one, weight_two)
    ))
    return jnp.maximum(second, 0.0)


def solution(mesh):
    placed = (
        P(("row", "col"), None),
        P("row", "col", None, None, None),
        P("row", "col", None, None),
        P(),
        P(),
        P(),
    )
    return jax.shard_map(
        functools.partial(shards, mesh.shape["row"], mesh.shape["col"]),
        mesh=mesh, in_specs=placed, out_specs=P(("row", "col"), None), check_vma=False,
    )
```

```python
import functools

import jax
import jax.numpy as jnp
from jax import lax
from jax.experimental import pallas as pl
from jax.experimental.pallas import tpu as pltpu
from jax.sharding import PartitionSpec as P

MESH = pl.DeviceIdType.MESH
PARTS = 4
LINK_TYPES = (jnp.int16, jnp.bfloat16)
TOP = 32766.0
LEAD = 3
FILL = 1


def kernel(
    n_row, n_col, blocks,
    counts_hbm, places_hbm, features_hbm, tiles_hbm, weight_one_hbm, weight_two_hbm,
    out_ref,
    tiles, dense, weights, inputs, total, prod, pair_in,
    out0, out1, land0, land1, via0, via1, scale_out, scale_land, scale_via,
    wave, load_sem, feature_sem, gather_send, gather_recv, pair_send, pair_recv,
    link_send, land_recv, via_recv, scale_send, scale_land_recv, scale_via_recv,
    counts, places, inverse_rows, inverse_ref,
):
    row, col = lax.axis_index("row"), lax.axis_index("col")
    n_chip = n_col // 2
    chip, core = col // 2, col % 2
    partner = chip * 2 + (1 - core)
    slots, tile = tiles_hbm.shape[0], tiles_hbm.shape[1]
    piece, width = features_hbm.shape
    part = width // PARTS
    sub = piece // blocks
    depth = piece * n_row
    tile_rows, tile_cols = dense.shape[0] // tile, depth // tile
    turns = n_chip - 1

    barrier = pltpu.get_barrier_semaphore()

    def beside(way):
        return (row, (chip + way) * 2 + core)

    @pl.when(chip > 0)
    def _():
        pl.semaphore_signal(barrier, inc=1, device_id=beside(-1), device_id_type=MESH)

    @pl.when(chip < n_chip - 1)
    def _():
        pl.semaphore_signal(barrier, inc=1, device_id=beside(1), device_id_type=MESH)

    for step in range(1, n_row):
        pl.semaphore_signal(
            barrier, inc=1, device_id=(lax.rem(row + step, n_row), col), device_id_type=MESH
        )
    pl.semaphore_signal(barrier, inc=1, device_id=(row, partner), device_id_type=MESH)

    def slot_rows(b, q):
        return pl.ds(pl.multiple_of((b * n_row + q) * sub, sub), sub)

    feature_loads = [
        [
            pltpu.make_async_copy(
                features_hbm.at[pl.ds(b * sub, sub), pl.ds(h * part, part)],
                inputs.at[0, h, slot_rows(b, row), :],
                feature_sem,
            )
            for b in range(blocks)
        ]
        for h in range(PARTS)
    ]
    for loads in feature_loads:
        for load in loads:
            load.start()
    peers = n_row + jnp.where(chip > 0, 1, 0) + jnp.where(chip < n_chip - 1, 1, 0)
    lower = chip < n_chip // 2
    end_chip = (chip == 0) | (chip == turns)
    neighbour = jnp.where(chip == 0, 1, turns - 1)

    def gather_copy(layer, b, h, step):
        block = inputs.at[layer, h, slot_rows(b, row), :]
        return pltpu.make_async_remote_copy(
            src_ref=block, dst_ref=block,
            send_sem=gather_send.at[layer], recv_sem=gather_recv.at[layer, b, h],
            device_id=(row ^ step, col), device_id_type=MESH,
        )

    def gather_start(layer, b, h):
        for step in reversed(range(1, n_row)):
            gather_copy(layer, b, h, step).start()

    def whole_wait(block, send_sem, recv_sem):
        return pltpu.make_async_remote_copy(
            src_ref=block, dst_ref=block, send_sem=send_sem, recv_sem=recv_sem,
            device_id=(row, partner), device_id_type=MESH,
        )

    def gather_wait(layer, b, h):
        block = inputs.at[layer, h, pl.ds(0, (n_row - 1) * sub), :]
        whole_wait(block, gather_send.at[layer], gather_recv.at[layer, b, h]).wait_recv()

    def pass_on(way, waits):
        at = 0 if way > 0 else 1
        if waits:
            pl.semaphore_wait(wave.at[at], 1)

        @pl.when((chip < n_chip - 1) if way > 0 else (chip > 0))
        def _():
            pl.semaphore_signal(wave.at[at], inc=1, device_id=beside(way), device_id_type=MESH)

    def pair_copy(layer, h, d):
        return pltpu.make_async_remote_copy(
            src_ref=prod.at[layer, h, d, 1 - core],
            dst_ref=pair_in.at[layer, h, d],
            send_sem=pair_send.at[layer], recv_sem=pair_recv.at[layer, h, d],
            device_id=(row, partner), device_id_type=MESH,
        )

    outs, lands, vias = (out0, out1), (land0, land1), (via0, via1)

    def spot_of(b, h, d):
        return (b * PARTS + h) * n_chip + d

    skipped = 2 if n_chip > 3 else 0

    def via_spot(b, h, d):
        spot = ((b - 1) * PARTS + h) * (n_chip - skipped)
        return spot + d - jnp.where(lower, skipped, 0)

    def link_copy(layer, b, h, d, target, scale, via):
        at, here = spot_of(b, h, d), spot_of(b, h, chip)
        if via:
            there = via_spot(b, h, d)
            place = (scale_via if scale else vias[layer]).at[there]
            recv = (scale_via_recv if scale else via_recv.at[layer]).at[there]
        else:
            place = (scale_land if scale else lands[layer]).at[here]
            recv = (scale_land_recv if scale else land_recv.at[layer]).at[b, chip]
        return pltpu.make_async_remote_copy(
            src_ref=(scale_out if scale else outs[layer]).at[at], dst_ref=place,
            send_sem=scale_send if scale else link_send.at[layer], recv_sem=recv,
            device_id=(row, target * 2 + core), device_id_type=MESH,
        )

    def both(layer):
        return (True, False) if LINK_TYPES[layer] == jnp.int16 else (False,)

    def post(layer, b, h, d, value):
        at = spot_of(b, h, d)
        if LINK_TYPES[layer] == jnp.int16:
            peak = jnp.maximum(jnp.max(jnp.abs(value), axis=0, keepdims=True), 1e-30)
            scale_out[at] = peak * (1.0 / TOP)
            outs[layer][at] = jnp.round(value * (TOP / peak)).astype(jnp.int32).astype(jnp.int16)
        else:
            outs[layer][at] = value.astype(outs[layer].dtype)
        if b == 0:
            for scale in both(layer):
                link_copy(layer, b, h, d, d, scale, False).start()
        else:
            detour = end_chip & (d != neighbour)

            @pl.when(detour)
            def _():
                for scale in both(layer):
                    link_copy(layer, b, h, d, neighbour, scale, True).start()

            @pl.when(jnp.logical_not(detour))
            def _():
                for scale in both(layer):
                    link_copy(layer, b, h, d, d, scale, False).start()

    def decode(layer, block, scale):
        if LINK_TYPES[layer] == jnp.int16:
            return block.astype(jnp.int32).astype(jnp.float32) * scale
        return block.astype(jnp.float32)

    def land_wait(layer, b, s):
        for scale in both(layer):
            whole_wait(
                (scale_land if scale else lands[layer]).at[pl.ds(0, PARTS)],
                scale_send if scale else link_send.at[layer],
                (scale_land_recv if scale else land_recv.at[layer]).at[b, s],
            ).wait_recv()

    def take_land(layer, b, h, s):
        at = spot_of(b, h, s)
        return decode(layer, lands[layer][at], scale_land[at])

    def take_via(layer, b, h, d):
        at = via_spot(b, h, d)
        for scale in both(layer):
            link_copy(layer, b, h, d, partner // 2, scale, True).wait_recv()
        return decode(layer, vias[layer][at], scale_via[at])

    def pair_sum(layer, b, h, d):
        rows = pl.ds(b * sub, sub)
        return prod[layer, h, d, core, rows, :] + pair_in[layer, h, d, rows, :]

    def send(layer, b, h, d):
        if b == 0:
            post(layer, b, h, d, pair_sum(layer, b, h, d))
        else:
            merged = ((chip == 1) & (d > 1)) | ((chip == turns - 1) & (d < turns - 1))

            @pl.when(merged)
            def _():
                post(layer, b, h, d, pair_sum(layer, b, h, d) + take_via(layer, b, h, d))

            @pl.when(jnp.logical_not(merged))
            def _():
                post(layer, b, h, d, pair_sum(layer, b, h, d))

    def sources(b, s):
        if b == 0:
            return s != chip
        first_hop = ((s == 0) & (chip != 1)) | ((s == turns) & (chip != turns - 1))
        return (s != chip) & jnp.logical_not(first_hop)

    def settle(layer, b):
        for h in range(PARTS):
            total[b, :, h * part : (h + 1) * part] = pair_sum(layer, b, h, chip)

        def add(i, carry):
            s = late_chip(i)

            @pl.when(sources(b, s))
            def _():
                land_wait(layer, b, s)
                for h in range(PARTS):
                    total[b, :, h * part : (h + 1) * part] += take_land(layer, b, h, s)

            return carry

        lax.fori_loop(0, n_chip, add, 0)

    def project(layer, b):
        return jnp.dot(
            total[b], weights[layer], precision=lax.Precision.HIGHEST,
            preferred_element_type=jnp.float32,
        )

    def chip_rows(d):
        return pl.ds(pl.multiple_of(d * (2 * piece), 2 * piece), 2 * piece)

    def unit_chip(i):
        return jnp.where(chip < n_chip // 2, turns - i, i)

    def late_chip(i):
        return jnp.where(
            chip < n_chip // 2, lax.rem(n_chip - i, n_chip), lax.rem(turns + i, n_chip)
        )

    early = depth - depth // blocks
    known_parts = PARTS // 2

    def unit(layer, u):
        h, i = u // n_chip, lax.rem(u, n_chip)
        split = layer == 1 and blocks > 1

        @pl.when(i == 0)
        def _():
            if split:
                @pl.when(h >= known_parts)
                def _():
                    gather_wait(layer, 0, h)

                gather_wait(layer, 1, h)
            else:
                for b in range(blocks):
                    gather_wait(layer, b, h)

            @pl.when(h + 2 < PARTS)
            def _():
                if split:
                    @pl.when(h + 2 >= known_parts)
                    def _():
                        gather_start(layer, 0, h + 2)

                    gather_start(layer, 1, h + 2)
                else:
                    for b in range(blocks):
                        gather_start(layer, b, h + 2)

        d = unit_chip(i)

        def whole():
            value = jnp.dot(
                dense[chip_rows(d), :], inputs[layer, h], preferred_element_type=jnp.float32
            )
            prod[layer, h, d] = value.reshape(2, piece, part)

        if split:
            @pl.when(h < known_parts)
            def _():
                value = jnp.dot(
                    dense[chip_rows(d), early:], inputs[layer, h, early:, :],
                    preferred_element_type=jnp.float32,
                )
                prod[layer, h, d] += value.reshape(2, piece, part)

            @pl.when(h >= known_parts)
            def _():
                whole()
        else:
            whole()
        pair_copy(layer, h, d).start()

    def early_unit(i):
        d = unit_chip(i)
        known = jnp.concatenate([inputs[1, h, 0:early, :] for h in range(known_parts)], axis=1)
        value = jnp.dot(dense[chip_rows(d), 0:early], known, preferred_element_type=jnp.float32)
        for h in range(known_parts):
            prod[1, h, d] = value[:, h * part : (h + 1) * part].reshape(2, piece, part)

    units = PARTS * n_chip

    def run_first(layer):
        def body(u, carry):
            k = u - LEAD

            @pl.when(k >= 0)
            def _():
                h, d = k // n_chip, unit_chip(lax.rem(k, n_chip))
                pair_copy(layer, h, d).wait_recv()

                @pl.when(d != chip)
                def _():
                    send(layer, 0, h, d)

                @pl.when((d != chip) & end_chip & (h < FILL))
                def _():
                    for b in range(1, blocks):
                        send(layer, b, h, d)

            @pl.when(u < units)
            def _():
                unit(layer, u)

            return carry

        lax.fori_loop(0, units + LEAD, body, 0)

    def run_merge(layer):
        def body(i, carry):
            d = late_chip(i)

            @pl.when((d != chip) & jnp.logical_not(end_chip))
            def _():
                for b in range(1, blocks):
                    for h in range(FILL):
                        send(layer, b, h, d)

            return carry

        if blocks > 1:
            lax.fori_loop(1, n_chip, body, 0)

    def run_rest(layer, begin, end):
        def body(w, carry):
            d, h = late_chip(w // PARTS), lax.rem(w, PARTS)

            @pl.when((d != chip) & ((h >= FILL) | ((w < PARTS) & jnp.logical_not(end_chip))))
            def _():
                for b in range(1, blocks):
                    send(layer, b, h, d)

            return carry

        if blocks > 1:
            lax.fori_loop(begin, end, body, 0)

    def hide(b):
        value = jnp.maximum(project(0, b), 0.0).astype(inputs.dtype)
        for h in range(PARTS):
            inputs[1, h, slot_rows(b, row), :] = value[:, h * part : (h + 1) * part]

    def drain(layer):
        sent = inputs.at[layer, :, pl.ds(0, depth // n_row * (n_row - 1)), :]
        whole_wait(sent, gather_send.at[layer], gather_recv.at[layer, 0, 0]).wait_send()
        whole_wait(
            pair_in.at[layer], pair_send.at[layer], pair_recv.at[layer, 0, 0]
        ).wait_send()
        for scale in both(layer):
            whole_wait(
                (scale_out if scale else outs[layer]).at[pl.ds(0, blocks * PARTS * turns)],
                scale_send if scale else link_send.at[layer],
                (scale_land_recv if scale else land_recv.at[layer]).at[0, 0],
            ).wait_send()

    own = inputs.at[0, :, pl.ds(0, piece), :]
    pltpu.make_async_copy(own, own, feature_sem).wait()
    counts_load = pltpu.make_async_copy(counts_hbm, counts, load_sem.at[4])
    counts_load.start()
    places_load = pltpu.make_async_copy(places_hbm, places, load_sem.at[5])
    places_load.start()
    tile_load = pltpu.make_async_copy(tiles_hbm, tiles.at[pl.ds(0, slots)], load_sem.at[0])
    tile_load.start()
    weight_loads = [
        pltpu.make_async_copy(weight_one_hbm, weights.at[0], load_sem.at[1]),
        pltpu.make_async_copy(weight_two_hbm, weights.at[1], load_sem.at[2]),
    ]
    for load in weight_loads:
        load.start()

    pl.semaphore_wait(barrier, peers)
    for b in range(blocks):
        gather_start(0, b, 0)

    @pl.when(chip == 0)
    def _():
        pass_on(1, False)

    @pl.when(chip == n_chip - 1)
    def _():
        pass_on(-1, False)

    tiles[slots] = jnp.zeros((tile, tile), tiles.dtype)
    spots = tile_rows * tile_cols
    counts_load.wait()
    places_load.wait()
    count = counts[row, col]
    order = lax.broadcasted_iota(jnp.int32, (spots, slots), 1)
    spot = lax.broadcasted_iota(jnp.int32, (spots, slots), 0)
    place = places[0:1, :] * tile_cols + places[1:2, :]
    listed = (place == spot) & (order < count)
    marks = jnp.where(listed, order - slots, 0)
    found = jnp.sum(marks.T, axis=0, keepdims=True) + slots
    inverse_rows[...] = jnp.broadcast_to(found, inverse_rows.shape)
    inverse_load = pltpu.make_async_copy(inverse_rows, inverse_ref, load_sem.at[3])
    inverse_load.start()
    inverse_load.wait()

    @pl.when(lower & (chip > 0))
    def _():
        pass_on(1, True)

    @pl.when(jnp.logical_not(lower) & (chip < n_chip - 1))
    def _():
        pass_on(-1, True)

    tile_load.wait()

    def place_row(i, carry):
        rows = pl.ds(pl.multiple_of(i * tile, tile), tile)
        for t in range(tile_cols):
            at = (t % blocks) * (tile_cols // blocks) + t // blocks
            slot = jnp.clip(inverse_ref[0, i * tile_cols + t], 0, slots)
            dense[rows, at * tile : (at + 1) * tile] = tiles[slot]
        return carry

    lax.fori_loop(0, tile_rows, place_row, 0)
    for b in range(blocks):
        gather_start(0, b, 1)

    @pl.when(lower)
    def _():
        pass_on(-1, True)

    @pl.when(jnp.logical_not(lower))
    def _():
        pass_on(1, True)

    for load in weight_loads:
        load.wait()

    middle = jnp.where(end_chip, units, units // 2)
    run_first(0)
    run_merge(0)
    run_rest(0, 0, middle)
    if blocks > 1:
        settle(0, 0)
        hide(0)
        for h in range(known_parts):
            gather_start(1, 0, h)
    run_rest(0, middle, units)
    settle(0, blocks - 1)
    hide(blocks - 1)
    gather_start(1, blocks - 1, 0)
    gather_start(1, blocks - 1, 1)
    if blocks > 1:
        for h in range(known_parts):
            gather_wait(1, 0, h)
        for i in range(n_chip):
            early_unit(i)

    run_first(1)
    run_merge(1)
    run_rest(1, 0, middle)
    drain(0)
    if blocks > 1:
        settle(1, 0)
        out_ref[0:sub, :] = project(1, 0)
    run_rest(1, middle, units)
    drain(1)
    settle(1, blocks - 1)
    out_ref[(blocks - 1) * sub :, :] = project(1, blocks - 1)


def shards(n_row, n_col, features, tile_values, tile_places, tile_counts, weight_one, weight_two):
    tiles = tile_values.reshape(tile_values.shape[2:])
    places = tile_places.reshape(tile_places.shape[2:])
    slots, tile = tiles.shape[0], tiles.shape[1]
    piece, width = features.shape
    part = width // PARTS
    blocks = 2 if piece == 2 * tile else 1
    sub = piece // blocks
    rows, depth = piece * n_col, piece * n_row
    tile_rows, tile_cols = rows // tile, depth // tile
    n_chip = n_col // 2
    spots = tile_rows * tile_cols
    items = blocks * PARTS * n_chip
    detours = max(1, (blocks - 1) * PARTS * (n_chip - 2 if n_chip > 3 else n_chip))

    def flow(layer, count):
        return pltpu.VMEM((count, sub, part), LINK_TYPES[layer])

    def scales(count):
        return pltpu.VMEM((count, 1, part), jnp.float32)

    dma = pltpu.SemaphoreType.DMA
    hbm = pl.BlockSpec(memory_space=pltpu.HBM)
    second = pl.pallas_call(
        functools.partial(kernel, n_row, n_col, blocks),
        out_shape=jax.ShapeDtypeStruct((piece, width), jnp.float32),
        in_specs=[hbm] * 6,
        out_specs=pl.BlockSpec(memory_space=pltpu.VMEM),
        scratch_shapes=[
            pltpu.VMEM((slots + 1, tile, tile), jnp.bfloat16),
            pltpu.VMEM((rows, depth), jnp.bfloat16),
            pltpu.VMEM((2, width, width), jnp.float32),
            pltpu.VMEM((2, PARTS, depth, part), jnp.bfloat16),
            pltpu.VMEM((blocks, sub, width), jnp.float32),
            pltpu.VMEM((2, PARTS, n_chip, 2, piece, part), jnp.float32),
            pltpu.VMEM((2, PARTS, n_chip, piece, part), jnp.float32),
            flow(0, items), flow(1, items), flow(0, items), flow(1, items),
            flow(0, detours), flow(1, detours),
            scales(items), scales(items), scales(detours),
            pltpu.SemaphoreType.REGULAR((2,)), dma((6,)), dma(()),
            dma((2,)), dma((2, blocks, PARTS)),
            dma((2,)), dma((2, PARTS, n_chip)),
            dma((2,)), dma((2, blocks, n_chip)), dma((2, detours)),
            dma(()), dma((blocks, n_chip)), dma((detours,)),
            pltpu.SMEM(tile_counts.shape, jnp.int32), pltpu.VMEM(places.shape, jnp.int32),
            pltpu.VMEM((8, spots), jnp.int32), pltpu.SMEM((8, spots), jnp.int32),
        ],
        compiler_params=pltpu.CompilerParams(
            collective_id=0, has_side_effects=True, vmem_limit_bytes=40 * 1024 * 1024
        ),
    )(*(
        pltpu.with_memory_space_constraint(x, pltpu.HBM)
        for x in (tile_counts, places, features, tiles, weight_one, weight_two)
    ))
    return jnp.maximum(second, 0.0)


def solution(mesh):
    placed = (
        P(("row", "col"), None),
        P("row", "col", None, None, None),
        P("row", "col", None, None),
        P(),
        P(),
        P(),
    )
    return jax.shard_map(
        functools.partial(shards, mesh.shape["row"], mesh.shape["col"]),
        mesh=mesh, in_specs=placed, out_specs=P(("row", "col"), None), check_vma=False,
    )
```

```python
import functools

import jax
import jax.numpy as jnp
from jax import lax
from jax.experimental import pallas as pl
from jax.experimental.pallas import tpu as pltpu
from jax.sharding import PartitionSpec as P

MESH = pl.DeviceIdType.MESH
PARTS = 4
LINK_TYPES = (jnp.int16, jnp.bfloat16)
TOP = 32766.0
LEAD = 3
FILL = 1


def kernel(
    n_row, n_col, blocks,
    counts_hbm, places_hbm, features_hbm, tiles_hbm, weight_one_hbm, weight_two_hbm,
    out_ref,
    tiles, dense, weights, inputs, total, prod, pair_in,
    out0, out1, land0, land1, via0, via1, scale_out, scale_land, scale_via,
    wave, load_sem, feature_sem, gather_send, gather_recv, pair_send, pair_recv,
    link_send, land_recv, via_recv, scale_send, scale_land_recv, scale_via_recv,
    counts, places, inverse_rows, inverse_ref,
):
    row, col = lax.axis_index("row"), lax.axis_index("col")
    n_chip = n_col // 2
    chip, core = col // 2, col % 2
    partner = chip * 2 + (1 - core)
    slots, tile = tiles_hbm.shape[0], tiles_hbm.shape[1]
    piece, width = features_hbm.shape
    part = width // PARTS
    sub = piece // blocks
    depth = piece * n_row
    tile_rows, tile_cols = dense.shape[0] // tile, depth // tile
    turns = n_chip - 1

    barrier = pltpu.get_barrier_semaphore()

    def beside(way):
        return (row, (chip + way) * 2 + core)

    @pl.when(chip > 0)
    def _():
        pl.semaphore_signal(barrier, inc=1, device_id=beside(-1), device_id_type=MESH)

    @pl.when(chip < n_chip - 1)
    def _():
        pl.semaphore_signal(barrier, inc=1, device_id=beside(1), device_id_type=MESH)

    for step in range(1, n_row):
        pl.semaphore_signal(
            barrier, inc=1, device_id=(lax.rem(row + step, n_row), col), device_id_type=MESH
        )
    pl.semaphore_signal(barrier, inc=1, device_id=(row, partner), device_id_type=MESH)

    def slot_rows(b, q):
        return pl.ds(pl.multiple_of((b * n_row + q) * sub, sub), sub)

    feature_loads = [
        [
            pltpu.make_async_copy(
                features_hbm.at[pl.ds(b * sub, sub), pl.ds(h * part, part)],
                inputs.at[0, h, slot_rows(b, row), :],
                feature_sem,
            )
            for b in range(blocks)
        ]
        for h in range(PARTS)
    ]
    for loads in feature_loads:
        for load in loads:
            load.start()
    peers = n_row + jnp.where(chip > 0, 1, 0) + jnp.where(chip < n_chip - 1, 1, 0)
    lower = chip < n_chip // 2
    end_chip = (chip == 0) | (chip == turns)
    neighbour = jnp.where(chip == 0, 1, turns - 1)

    def gather_copy(layer, b, h, step):
        block = inputs.at[layer, h, slot_rows(b, row), :]
        return pltpu.make_async_remote_copy(
            src_ref=block, dst_ref=block,
            send_sem=gather_send.at[layer], recv_sem=gather_recv.at[layer, b, h],
            device_id=(row ^ step, col), device_id_type=MESH,
        )

    def gather_start(layer, b, h):
        for step in reversed(range(1, n_row)):
            gather_copy(layer, b, h, step).start()

    def whole_wait(block, send_sem, recv_sem):
        return pltpu.make_async_remote_copy(
            src_ref=block, dst_ref=block, send_sem=send_sem, recv_sem=recv_sem,
            device_id=(row, partner), device_id_type=MESH,
        )

    def gather_wait(layer, b, h):
        block = inputs.at[layer, h, pl.ds(0, (n_row - 1) * sub), :]
        whole_wait(block, gather_send.at[layer], gather_recv.at[layer, b, h]).wait_recv()

    def pass_on(way, waits):
        at = 0 if way > 0 else 1
        if waits:
            pl.semaphore_wait(wave.at[at], 1)

        @pl.when((chip < n_chip - 1) if way > 0 else (chip > 0))
        def _():
            pl.semaphore_signal(wave.at[at], inc=1, device_id=beside(way), device_id_type=MESH)

    def pair_copy(layer, h, d):
        return pltpu.make_async_remote_copy(
            src_ref=prod.at[layer, h, d, 1 - core],
            dst_ref=pair_in.at[layer, h, d],
            send_sem=pair_send.at[layer], recv_sem=pair_recv.at[layer, h, d],
            device_id=(row, partner), device_id_type=MESH,
        )

    outs, lands, vias = (out0, out1), (land0, land1), (via0, via1)

    def spot_of(b, h, d):
        return (b * PARTS + h) * n_chip + d

    skipped = 2 if n_chip > 3 else 0

    def via_spot(b, h, d):
        spot = ((b - 1) * PARTS + h) * (n_chip - skipped)
        return spot + d - jnp.where(lower, skipped, 0)

    def link_copy(layer, b, h, d, target, scale, via):
        at, here = spot_of(b, h, d), spot_of(b, h, chip)
        if via:
            there = via_spot(b, h, d)
            place = (scale_via if scale else vias[layer]).at[there]
            recv = (scale_via_recv if scale else via_recv.at[layer]).at[there]
        else:
            place = (scale_land if scale else lands[layer]).at[here]
            recv = (scale_land_recv if scale else land_recv.at[layer]).at[b, chip]
        return pltpu.make_async_remote_copy(
            src_ref=(scale_out if scale else outs[layer]).at[at], dst_ref=place,
            send_sem=scale_send if scale else link_send.at[layer], recv_sem=recv,
            device_id=(row, target * 2 + core), device_id_type=MESH,
        )

    def both(layer):
        return (True, False) if LINK_TYPES[layer] == jnp.int16 else (False,)

    def post(layer, b, h, d, value):
        at = spot_of(b, h, d)
        if LINK_TYPES[layer] == jnp.int16:
            peak = jnp.maximum(jnp.max(jnp.abs(value), axis=0, keepdims=True), 1e-30)
            scale_out[at] = peak * (1.0 / TOP)
            outs[layer][at] = jnp.round(value * (TOP / peak)).astype(jnp.int32).astype(jnp.int16)
        else:
            outs[layer][at] = value.astype(outs[layer].dtype)
        if b == 0:
            for scale in both(layer):
                link_copy(layer, b, h, d, d, scale, False).start()
        else:
            detour = end_chip & (d != neighbour)

            @pl.when(detour)
            def _():
                for scale in both(layer):
                    link_copy(layer, b, h, d, neighbour, scale, True).start()

            @pl.when(jnp.logical_not(detour))
            def _():
                for scale in both(layer):
                    link_copy(layer, b, h, d, d, scale, False).start()

    def decode(layer, block, scale):
        if LINK_TYPES[layer] == jnp.int16:
            return block.astype(jnp.int32).astype(jnp.float32) * scale
        return block.astype(jnp.float32)

    def land_wait(layer, b, s):
        for scale in both(layer):
            whole_wait(
                (scale_land if scale else lands[layer]).at[pl.ds(0, PARTS)],
                scale_send if scale else link_send.at[layer],
                (scale_land_recv if scale else land_recv.at[layer]).at[b, s],
            ).wait_recv()

    def take_land(layer, b, h, s):
        at = spot_of(b, h, s)
        return decode(layer, lands[layer][at], scale_land[at])

    def take_via(layer, b, h, d):
        at = via_spot(b, h, d)
        for scale in both(layer):
            link_copy(layer, b, h, d, partner // 2, scale, True).wait_recv()
        return decode(layer, vias[layer][at], scale_via[at])

    def pair_sum(layer, b, h, d):
        rows = pl.ds(b * sub, sub)
        return prod[layer, h, d, core, rows, :] + pair_in[layer, h, d, rows, :]

    def send(layer, b, h, d):
        if b == 0:
            post(layer, b, h, d, pair_sum(layer, b, h, d))
        else:
            merged = ((chip == 1) & (d > 1)) | ((chip == turns - 1) & (d < turns - 1))

            @pl.when(merged)
            def _():
                post(layer, b, h, d, pair_sum(layer, b, h, d) + take_via(layer, b, h, d))

            @pl.when(jnp.logical_not(merged))
            def _():
                post(layer, b, h, d, pair_sum(layer, b, h, d))

    def sources(b, s):
        if b == 0:
            return s != chip
        first_hop = ((s == 0) & (chip != 1)) | ((s == turns) & (chip != turns - 1))
        return (s != chip) & jnp.logical_not(first_hop)

    def settle(layer, b):
        for h in range(PARTS):
            total[b, :, h * part : (h + 1) * part] = pair_sum(layer, b, h, chip)

        def add(i, carry):
            s = late_chip(i)

            @pl.when(sources(b, s))
            def _():
                land_wait(layer, b, s)
                for h in range(PARTS):
                    total[b, :, h * part : (h + 1) * part] += take_land(layer, b, h, s)

            return carry

        lax.fori_loop(0, n_chip, add, 0)

    def project(layer, b):
        return jnp.dot(
            total[b], weights[layer], precision=lax.Precision.HIGHEST,
            preferred_element_type=jnp.float32,
        )

    def chip_rows(d):
        return pl.ds(pl.multiple_of(d * (2 * piece), 2 * piece), 2 * piece)

    def unit_chip(i):
        return jnp.where(chip < n_chip // 2, turns - i, i)

    def late_chip(i):
        return jnp.where(
            chip < n_chip // 2, lax.rem(n_chip - i, n_chip), lax.rem(turns + i, n_chip)
        )

    early = depth - depth // blocks
    known_parts = PARTS // 2

    def unit(layer, u):
        h, i = u // n_chip, lax.rem(u, n_chip)
        split = layer == 1 and blocks > 1

        @pl.when(i == 0)
        def _():
            if split:
                @pl.when(h >= known_parts)
                def _():
                    gather_wait(layer, 0, h)

                gather_wait(layer, 1, h)
            else:
                for b in range(blocks):
                    gather_wait(layer, b, h)

            @pl.when(h + 2 < PARTS)
            def _():
                if split:
                    @pl.when(h + 2 >= known_parts)
                    def _():
                        gather_start(layer, 0, h + 2)

                    gather_start(layer, 1, h + 2)
                else:
                    for b in range(blocks):
                        gather_start(layer, b, h + 2)

        d = unit_chip(i)

        def whole():
            value = jnp.dot(
                dense[chip_rows(d), :], inputs[layer, h], preferred_element_type=jnp.float32
            )
            prod[layer, h, d] = value.reshape(2, piece, part)

        if split:
            @pl.when(h < known_parts)
            def _():
                value = jnp.dot(
                    dense[chip_rows(d), early:], inputs[layer, h, early:, :],
                    preferred_element_type=jnp.float32,
                )
                prod[layer, h, d] += value.reshape(2, piece, part)

            @pl.when(h >= known_parts)
            def _():
                whole()
        else:
            whole()
        pair_copy(layer, h, d).start()

    def early_unit(i):
        d = unit_chip(i)
        known = jnp.concatenate([inputs[1, h, 0:early, :] for h in range(known_parts)], axis=1)
        value = jnp.dot(dense[chip_rows(d), 0:early], known, preferred_element_type=jnp.float32)
        for h in range(known_parts):
            prod[1, h, d] = value[:, h * part : (h + 1) * part].reshape(2, piece, part)

    units = PARTS * n_chip

    def run_first(layer):
        def body(u, carry):
            k = u - LEAD

            @pl.when(k >= 0)
            def _():
                h, d = k // n_chip, unit_chip(lax.rem(k, n_chip))
                pair_copy(layer, h, d).wait_recv()

                @pl.when(d != chip)
                def _():
                    send(layer, 0, h, d)

                @pl.when((d != chip) & end_chip & (h < FILL))
                def _():
                    for b in range(1, blocks):
                        send(layer, b, h, d)

            @pl.when(u < units)
            def _():
                unit(layer, u)

            return carry

        lax.fori_loop(0, units + LEAD, body, 0)

    def run_merge(layer):
        def body(i, carry):
            d = late_chip(i)

            @pl.when((d != chip) & jnp.logical_not(end_chip))
            def _():
                for b in range(1, blocks):
                    for h in range(FILL):
                        send(layer, b, h, d)

            return carry

        if blocks > 1:
            lax.fori_loop(1, n_chip, body, 0)

    def run_rest(layer, begin, end):
        def body(w, carry):
            d, h = late_chip(w // PARTS), lax.rem(w, PARTS)

            @pl.when((d != chip) & ((h >= FILL) | ((w < PARTS) & jnp.logical_not(end_chip))))
            def _():
                for b in range(1, blocks):
                    send(layer, b, h, d)

            return carry

        if blocks > 1:
            lax.fori_loop(begin, end, body, 0)

    def hide(b):
        value = jnp.maximum(project(0, b), 0.0).astype(inputs.dtype)
        for h in range(PARTS):
            inputs[1, h, slot_rows(b, row), :] = value[:, h * part : (h + 1) * part]

    def drain(layer):
        sent = inputs.at[layer, :, pl.ds(0, depth // n_row * (n_row - 1)), :]
        whole_wait(sent, gather_send.at[layer], gather_recv.at[layer, 0, 0]).wait_send()
        whole_wait(
            pair_in.at[layer], pair_send.at[layer], pair_recv.at[layer, 0, 0]
        ).wait_send()
        for scale in both(layer):
            whole_wait(
                (scale_out if scale else outs[layer]).at[pl.ds(0, blocks * PARTS * turns)],
                scale_send if scale else link_send.at[layer],
                (scale_land_recv if scale else land_recv.at[layer]).at[0, 0],
            ).wait_send()

    own = inputs.at[0, :, pl.ds(0, piece), :]
    pltpu.make_async_copy(own, own, feature_sem).wait()
    counts_load = pltpu.make_async_copy(counts_hbm, counts, load_sem.at[4])
    counts_load.start()
    places_load = pltpu.make_async_copy(places_hbm, places, load_sem.at[5])
    places_load.start()
    tile_load = pltpu.make_async_copy(tiles_hbm, tiles.at[pl.ds(0, slots)], load_sem.at[0])
    tile_load.start()
    weight_loads = [
        pltpu.make_async_copy(weight_one_hbm, weights.at[0], load_sem.at[1]),
        pltpu.make_async_copy(weight_two_hbm, weights.at[1], load_sem.at[2]),
    ]
    for load in weight_loads:
        load.start()

    pl.semaphore_wait(barrier, peers)
    for b in range(blocks):
        gather_start(0, b, 0)

    @pl.when(chip == 0)
    def _():
        pass_on(1, False)

    @pl.when(chip == n_chip - 1)
    def _():
        pass_on(-1, False)

    tiles[slots] = jnp.zeros((tile, tile), tiles.dtype)
    spots = tile_rows * tile_cols
    counts_load.wait()
    places_load.wait()
    count = counts[row, col]
    order = lax.broadcasted_iota(jnp.int32, (spots, slots), 1)
    spot = lax.broadcasted_iota(jnp.int32, (spots, slots), 0)
    place = places[0:1, :] * tile_cols + places[1:2, :]
    listed = (place == spot) & (order < count)
    marks = jnp.where(listed, order - slots, 0)
    found = jnp.sum(marks.T, axis=0, keepdims=True) + slots
    inverse_rows[...] = jnp.broadcast_to(found, inverse_rows.shape)
    inverse_load = pltpu.make_async_copy(inverse_rows, inverse_ref, load_sem.at[3])
    inverse_load.start()
    inverse_load.wait()

    @pl.when(lower & (chip > 0))
    def _():
        pass_on(1, True)

    @pl.when(jnp.logical_not(lower) & (chip < n_chip - 1))
    def _():
        pass_on(-1, True)

    tile_load.wait()

    def place_row(i, carry):
        rows = pl.ds(pl.multiple_of(i * tile, tile), tile)
        for t in range(tile_cols):
            at = (t % blocks) * (tile_cols // blocks) + t // blocks
            slot = jnp.clip(inverse_ref[0, i * tile_cols + t], 0, slots)
            dense[rows, at * tile : (at + 1) * tile] = tiles[slot]
        return carry

    lax.fori_loop(0, tile_rows, place_row, 0)
    for b in range(blocks):
        gather_start(0, b, 1)

    @pl.when(lower)
    def _():
        pass_on(-1, True)

    @pl.when(jnp.logical_not(lower))
    def _():
        pass_on(1, True)

    for load in weight_loads:
        load.wait()

    middle = jnp.where(end_chip, units, units // 2)
    run_first(0)
    run_merge(0)
    run_rest(0, 0, middle)
    if blocks > 1:
        settle(0, 0)
        hide(0)
        for h in range(known_parts):
            gather_start(1, 0, h)
    run_rest(0, middle, units)
    settle(0, blocks - 1)
    hide(blocks - 1)
    gather_start(1, blocks - 1, 0)
    gather_start(1, blocks - 1, 1)
    if blocks > 1:
        for h in range(known_parts):
            gather_wait(1, 0, h)
        for i in range(n_chip):
            early_unit(i)

    run_first(1)
    run_merge(1)
    run_rest(1, 0, units)
    drain(0)
    if blocks > 1:
        settle(1, 0)
        out_ref[0:sub, :] = project(1, 0)
    drain(1)
    settle(1, blocks - 1)
    out_ref[(blocks - 1) * sub :, :] = project(1, blocks - 1)


def shards(n_row, n_col, features, tile_values, tile_places, tile_counts, weight_one, weight_two):
    tiles = tile_values.reshape(tile_values.shape[2:])
    places = tile_places.reshape(tile_places.shape[2:])
    slots, tile = tiles.shape[0], tiles.shape[1]
    piece, width = features.shape
    part = width // PARTS
    blocks = 2 if piece == 2 * tile else 1
    sub = piece // blocks
    rows, depth = piece * n_col, piece * n_row
    tile_rows, tile_cols = rows // tile, depth // tile
    n_chip = n_col // 2
    spots = tile_rows * tile_cols
    items = blocks * PARTS * n_chip
    detours = max(1, (blocks - 1) * PARTS * (n_chip - 2 if n_chip > 3 else n_chip))

    def flow(layer, count):
        return pltpu.VMEM((count, sub, part), LINK_TYPES[layer])

    def scales(count):
        return pltpu.VMEM((count, 1, part), jnp.float32)

    dma = pltpu.SemaphoreType.DMA
    hbm = pl.BlockSpec(memory_space=pltpu.HBM)
    second = pl.pallas_call(
        functools.partial(kernel, n_row, n_col, blocks),
        out_shape=jax.ShapeDtypeStruct((piece, width), jnp.float32),
        in_specs=[hbm] * 6,
        out_specs=pl.BlockSpec(memory_space=pltpu.VMEM),
        scratch_shapes=[
            pltpu.VMEM((slots + 1, tile, tile), jnp.bfloat16),
            pltpu.VMEM((rows, depth), jnp.bfloat16),
            pltpu.VMEM((2, width, width), jnp.float32),
            pltpu.VMEM((2, PARTS, depth, part), jnp.bfloat16),
            pltpu.VMEM((blocks, sub, width), jnp.float32),
            pltpu.VMEM((2, PARTS, n_chip, 2, piece, part), jnp.float32),
            pltpu.VMEM((2, PARTS, n_chip, piece, part), jnp.float32),
            flow(0, items), flow(1, items), flow(0, items), flow(1, items),
            flow(0, detours), flow(1, detours),
            scales(items), scales(items), scales(detours),
            pltpu.SemaphoreType.REGULAR((2,)), dma((6,)), dma(()),
            dma((2,)), dma((2, blocks, PARTS)),
            dma((2,)), dma((2, PARTS, n_chip)),
            dma((2,)), dma((2, blocks, n_chip)), dma((2, detours)),
            dma(()), dma((blocks, n_chip)), dma((detours,)),
            pltpu.SMEM(tile_counts.shape, jnp.int32), pltpu.VMEM(places.shape, jnp.int32),
            pltpu.VMEM((8, spots), jnp.int32), pltpu.SMEM((8, spots), jnp.int32),
        ],
        compiler_params=pltpu.CompilerParams(
            collective_id=0, has_side_effects=True, vmem_limit_bytes=40 * 1024 * 1024
        ),
    )(*(
        pltpu.with_memory_space_constraint(x, pltpu.HBM)
        for x in (tile_counts, places, features, tiles, weight_one, weight_two)
    ))
    return jnp.maximum(second, 0.0)


def solution(mesh):
    placed = (
        P(("row", "col"), None),
        P("row", "col", None, None, None),
        P("row", "col", None, None),
        P(),
        P(),
        P(),
    )
    return jax.shard_map(
        functools.partial(shards, mesh.shape["row"], mesh.shape["col"]),
        mesh=mesh, in_specs=placed, out_specs=P(("row", "col"), None), check_vma=False,
    )
```

```python
import functools

import jax
import jax.numpy as jnp
from jax import lax
from jax.experimental import pallas as pl
from jax.experimental.pallas import tpu as pltpu
from jax.sharding import PartitionSpec as P

MESH = pl.DeviceIdType.MESH
PARTS = 4
LINK_TYPES = (jnp.int16, jnp.bfloat16)
TOP = 32766.0
LEAD = 3
FILL = 1


def kernel(
    n_row, n_col, blocks,
    counts_hbm, places_hbm, features_hbm, tiles_hbm, weight_one_hbm, weight_two_hbm,
    out_ref,
    tiles, dense, weights, inputs, total, prod, pair_in,
    out0, out1, land0, land1, via0, via1, scale_out, scale_land, scale_via,
    wave, load_sem, feature_sem, gather_send, gather_recv, pair_send, pair_recv,
    link_send, land_recv, via_recv, scale_send, scale_land_recv, scale_via_recv,
    counts, places, inverse_rows, inverse_ref,
):
    row, col = lax.axis_index("row"), lax.axis_index("col")
    n_chip = n_col // 2
    chip, core = col // 2, col % 2
    partner = chip * 2 + (1 - core)
    slots, tile = tiles_hbm.shape[0], tiles_hbm.shape[1]
    piece, width = features_hbm.shape
    part = width // PARTS
    sub = piece // blocks
    depth = piece * n_row
    tile_rows, tile_cols = dense.shape[0] // tile, depth // tile
    turns = n_chip - 1

    barrier = pltpu.get_barrier_semaphore()

    def beside(way):
        return (row, (chip + way) * 2 + core)

    @pl.when(chip > 0)
    def _():
        pl.semaphore_signal(barrier, inc=1, device_id=beside(-1), device_id_type=MESH)

    @pl.when(chip < n_chip - 1)
    def _():
        pl.semaphore_signal(barrier, inc=1, device_id=beside(1), device_id_type=MESH)

    for step in range(1, n_row):
        pl.semaphore_signal(
            barrier, inc=1, device_id=(lax.rem(row + step, n_row), col), device_id_type=MESH
        )
    pl.semaphore_signal(barrier, inc=1, device_id=(row, partner), device_id_type=MESH)

    def slot_rows(b, q):
        return pl.ds(pl.multiple_of((b * n_row + q) * sub, sub), sub)

    feature_loads = [
        [
            pltpu.make_async_copy(
                features_hbm.at[pl.ds(b * sub, sub), pl.ds(h * part, part)],
                inputs.at[0, h, slot_rows(b, row), :],
                feature_sem,
            )
            for b in range(blocks)
        ]
        for h in range(PARTS)
    ]
    for loads in feature_loads:
        for load in loads:
            load.start()
    peers = n_row + jnp.where(chip > 0, 1, 0) + jnp.where(chip < n_chip - 1, 1, 0)
    lower = chip < n_chip // 2
    end_chip = (chip == 0) | (chip == turns)
    neighbour = jnp.where(chip == 0, 1, turns - 1)

    def gather_copy(layer, b, h, step):
        block = inputs.at[layer, h, slot_rows(b, row), :]
        return pltpu.make_async_remote_copy(
            src_ref=block, dst_ref=block,
            send_sem=gather_send.at[layer], recv_sem=gather_recv.at[layer, b, h],
            device_id=(row ^ step, col), device_id_type=MESH,
        )

    def gather_start(layer, b, h):
        for step in reversed(range(1, n_row)):
            gather_copy(layer, b, h, step).start()

    def whole_wait(block, send_sem, recv_sem):
        return pltpu.make_async_remote_copy(
            src_ref=block, dst_ref=block, send_sem=send_sem, recv_sem=recv_sem,
            device_id=(row, partner), device_id_type=MESH,
        )

    def gather_wait(layer, b, h):
        block = inputs.at[layer, h, pl.ds(0, (n_row - 1) * sub), :]
        whole_wait(block, gather_send.at[layer], gather_recv.at[layer, b, h]).wait_recv()

    def pass_on(way, waits):
        at = 0 if way > 0 else 1
        if waits:
            pl.semaphore_wait(wave.at[at], 1)

        @pl.when((chip < n_chip - 1) if way > 0 else (chip > 0))
        def _():
            pl.semaphore_signal(wave.at[at], inc=1, device_id=beside(way), device_id_type=MESH)

    def pair_copy(layer, h, d):
        return pltpu.make_async_remote_copy(
            src_ref=prod.at[layer, h, d, 1 - core],
            dst_ref=pair_in.at[layer, h, d],
            send_sem=pair_send.at[layer], recv_sem=pair_recv.at[layer, h, d],
            device_id=(row, partner), device_id_type=MESH,
        )

    outs, lands, vias = (out0, out1), (land0, land1), (via0, via1)

    def spot_of(b, h, d):
        return (b * PARTS + h) * n_chip + d

    skipped = 2 if n_chip > 3 else 0

    def via_spot(b, h, d):
        spot = ((b - 1) * PARTS + h) * (n_chip - skipped)
        return spot + d - jnp.where(lower, skipped, 0)

    def link_copy(layer, b, h, d, target, scale, via):
        at, here = spot_of(b, h, d), spot_of(b, h, chip)
        if via:
            there = via_spot(b, h, d)
            place = (scale_via if scale else vias[layer]).at[there]
            recv = (scale_via_recv if scale else via_recv.at[layer]).at[there]
        else:
            place = (scale_land if scale else lands[layer]).at[here]
            recv = (scale_land_recv if scale else land_recv.at[layer]).at[0 if b == 0 else 1 + (b - 1) * n_chip + chip]
        return pltpu.make_async_remote_copy(
            src_ref=(scale_out if scale else outs[layer]).at[at], dst_ref=place,
            send_sem=scale_send if scale else link_send.at[layer], recv_sem=recv,
            device_id=(row, target * 2 + core), device_id_type=MESH,
        )

    def both(layer):
        return (True, False) if LINK_TYPES[layer] == jnp.int16 else (False,)

    def post(layer, b, h, d, value):
        at = spot_of(b, h, d)
        if LINK_TYPES[layer] == jnp.int16:
            peak = jnp.maximum(jnp.max(jnp.abs(value), axis=0, keepdims=True), 1e-30)
            scale_out[at] = peak * (1.0 / TOP)
            outs[layer][at] = jnp.round(value * (TOP / peak)).astype(jnp.int32).astype(jnp.int16)
        else:
            outs[layer][at] = value.astype(outs[layer].dtype)
        if b == 0:
            for scale in both(layer):
                link_copy(layer, b, h, d, d, scale, False).start()
        else:
            detour = end_chip & (d != neighbour)

            @pl.when(detour)
            def _():
                for scale in both(layer):
                    link_copy(layer, b, h, d, neighbour, scale, True).start()

            @pl.when(jnp.logical_not(detour))
            def _():
                for scale in both(layer):
                    link_copy(layer, b, h, d, d, scale, False).start()

    def decode(layer, block, scale):
        if LINK_TYPES[layer] == jnp.int16:
            return block.astype(jnp.int32).astype(jnp.float32) * scale
        return block.astype(jnp.float32)

    def land_wait(layer, b, s):
        for scale in both(layer):
            whole_wait(
                (scale_land if scale else lands[layer]).at[
                    pl.ds(0, PARTS * turns if b == 0 else PARTS)
                ],
                scale_send if scale else link_send.at[layer],
                (scale_land_recv if scale else land_recv.at[layer]).at[
                    0 if b == 0 else 1 + (b - 1) * n_chip + s
                ],
            ).wait_recv()

    def take_land(layer, b, h, s):
        at = spot_of(b, h, s)
        return decode(layer, lands[layer][at], scale_land[at])

    def take_via(layer, b, h, d):
        at = via_spot(b, h, d)
        for scale in both(layer):
            link_copy(layer, b, h, d, partner // 2, scale, True).wait_recv()
        return decode(layer, vias[layer][at], scale_via[at])

    def pair_sum(layer, b, h, d):
        rows = pl.ds(b * sub, sub)
        return prod[layer, h, d, core, rows, :] + pair_in[layer, h, d, rows, :]

    def send(layer, b, h, d):
        if b == 0:
            post(layer, b, h, d, pair_sum(layer, b, h, d))
        else:
            merged = ((chip == 1) & (d > 1)) | ((chip == turns - 1) & (d < turns - 1))

            @pl.when(merged)
            def _():
                post(layer, b, h, d, pair_sum(layer, b, h, d) + take_via(layer, b, h, d))

            @pl.when(jnp.logical_not(merged))
            def _():
                post(layer, b, h, d, pair_sum(layer, b, h, d))

    def sources(b, s):
        if b == 0:
            return s != chip
        first_hop = ((s == 0) & (chip != 1)) | ((s == turns) & (chip != turns - 1))
        return (s != chip) & jnp.logical_not(first_hop)

    def settle(layer, b):
        for h in range(PARTS):
            total[b, :, h * part : (h + 1) * part] = pair_sum(layer, b, h, chip)

        if b == 0:
            land_wait(layer, b, 0)

        def add(i, carry):
            s = late_chip(i)

            @pl.when(sources(b, s))
            def _():
                if b > 0:
                    land_wait(layer, b, s)
                for h in range(PARTS):
                    total[b, :, h * part : (h + 1) * part] += take_land(layer, b, h, s)

            return carry

        lax.fori_loop(0, n_chip, add, 0)

    def project(layer, b):
        return jnp.dot(
            total[b], weights[layer], precision=lax.Precision.HIGHEST,
            preferred_element_type=jnp.float32,
        )

    def chip_rows(d):
        return pl.ds(pl.multiple_of(d * (2 * piece), 2 * piece), 2 * piece)

    def unit_chip(i):
        return jnp.where(chip < n_chip // 2, turns - i, i)

    def late_chip(i):
        return jnp.where(
            chip < n_chip // 2, lax.rem(n_chip - i, n_chip), lax.rem(turns + i, n_chip)
        )

    early = depth - depth // blocks
    known_parts = PARTS // 2

    def unit(layer, u):
        h, i = u // n_chip, lax.rem(u, n_chip)
        split = layer == 1 and blocks > 1

        @pl.when(i == 0)
        def _():
            if split:
                @pl.when(h >= known_parts)
                def _():
                    gather_wait(layer, 0, h)

                gather_wait(layer, 1, h)
            else:
                for b in range(blocks):
                    gather_wait(layer, b, h)

            @pl.when(h + 2 < PARTS)
            def _():
                if split:
                    @pl.when(h + 2 >= known_parts)
                    def _():
                        gather_start(layer, 0, h + 2)

                    gather_start(layer, 1, h + 2)
                else:
                    for b in range(blocks):
                        gather_start(layer, b, h + 2)

        d = unit_chip(i)

        def whole():
            value = jnp.dot(
                dense[chip_rows(d), :], inputs[layer, h], preferred_element_type=jnp.float32
            )
            prod[layer, h, d] = value.reshape(2, piece, part)

        if split:
            @pl.when(h < known_parts)
            def _():
                value = jnp.dot(
                    dense[chip_rows(d), early:], inputs[layer, h, early:, :],
                    preferred_element_type=jnp.float32,
                )
                prod[layer, h, d] += value.reshape(2, piece, part)

            @pl.when(h >= known_parts)
            def _():
                whole()
        else:
            whole()
        pair_copy(layer, h, d).start()

    def early_unit(i):
        d = unit_chip(i)
        known = jnp.concatenate([inputs[1, h, 0:early, :] for h in range(known_parts)], axis=1)
        value = jnp.dot(dense[chip_rows(d), 0:early], known, preferred_element_type=jnp.float32)
        for h in range(known_parts):
            prod[1, h, d] = value[:, h * part : (h + 1) * part].reshape(2, piece, part)

    units = PARTS * n_chip

    def run_first(layer):
        def body(u, carry):
            k = u - LEAD

            @pl.when(k >= 0)
            def _():
                h, d = k // n_chip, unit_chip(lax.rem(k, n_chip))
                pair_copy(layer, h, d).wait_recv()

                @pl.when(d != chip)
                def _():
                    send(layer, 0, h, d)

                @pl.when((d != chip) & end_chip & (h < FILL))
                def _():
                    for b in range(1, blocks):
                        send(layer, b, h, d)

            @pl.when(u < units)
            def _():
                unit(layer, u)

            return carry

        lax.fori_loop(0, units + LEAD, body, 0)

    def run_merge(layer):
        def body(i, carry):
            d = late_chip(i)

            @pl.when((d != chip) & jnp.logical_not(end_chip))
            def _():
                for b in range(1, blocks):
                    for h in range(FILL):
                        send(layer, b, h, d)

            return carry

        if blocks > 1:
            lax.fori_loop(1, n_chip, body, 0)

    def run_rest(layer, begin, end):
        def body(w, carry):
            d, h = late_chip(w // PARTS), lax.rem(w, PARTS)

            @pl.when((d != chip) & ((h >= FILL) | ((w < PARTS) & jnp.logical_not(end_chip))))
            def _():
                for b in range(1, blocks):
                    send(layer, b, h, d)

            return carry

        if blocks > 1:
            lax.fori_loop(begin, end, body, 0)

    def hide(b):
        value = jnp.maximum(project(0, b), 0.0).astype(inputs.dtype)
        for h in range(PARTS):
            inputs[1, h, slot_rows(b, row), :] = value[:, h * part : (h + 1) * part]

    def drain(layer):
        sent = inputs.at[layer, :, pl.ds(0, depth // n_row * (n_row - 1)), :]
        whole_wait(sent, gather_send.at[layer], gather_recv.at[layer, 0, 0]).wait_send()
        whole_wait(
            pair_in.at[layer], pair_send.at[layer], pair_recv.at[layer, 0, 0]
        ).wait_send()
        for scale in both(layer):
            whole_wait(
                (scale_out if scale else outs[layer]).at[pl.ds(0, blocks * PARTS * turns)],
                scale_send if scale else link_send.at[layer],
                (scale_land_recv if scale else land_recv.at[layer]).at[0],
            ).wait_send()

    own = inputs.at[0, :, pl.ds(0, piece), :]
    pltpu.make_async_copy(own, own, feature_sem).wait()
    counts_load = pltpu.make_async_copy(counts_hbm, counts, load_sem.at[4])
    counts_load.start()
    places_load = pltpu.make_async_copy(places_hbm, places, load_sem.at[5])
    places_load.start()
    tile_load = pltpu.make_async_copy(tiles_hbm, tiles.at[pl.ds(0, slots)], load_sem.at[0])
    tile_load.start()
    weight_loads = [
        pltpu.make_async_copy(weight_one_hbm, weights.at[0], load_sem.at[1]),
        pltpu.make_async_copy(weight_two_hbm, weights.at[1], load_sem.at[2]),
    ]
    for load in weight_loads:
        load.start()

    pl.semaphore_wait(barrier, peers)
    for b in range(blocks):
        gather_start(0, b, 0)

    @pl.when(chip == 0)
    def _():
        pass_on(1, False)

    @pl.when(chip == n_chip - 1)
    def _():
        pass_on(-1, False)

    tiles[slots] = jnp.zeros((tile, tile), tiles.dtype)
    spots = tile_rows * tile_cols
    counts_load.wait()
    places_load.wait()
    count = counts[row, col]
    order = lax.broadcasted_iota(jnp.int32, (spots, slots), 1)
    spot = lax.broadcasted_iota(jnp.int32, (spots, slots), 0)
    place = places[0:1, :] * tile_cols + places[1:2, :]
    listed = (place == spot) & (order < count)
    marks = jnp.where(listed, order - slots, 0)
    found = jnp.sum(marks.T, axis=0, keepdims=True) + slots
    inverse_rows[...] = jnp.broadcast_to(found, inverse_rows.shape)
    inverse_load = pltpu.make_async_copy(inverse_rows, inverse_ref, load_sem.at[3])
    inverse_load.start()
    inverse_load.wait()

    @pl.when(lower & (chip > 0))
    def _():
        pass_on(1, True)

    @pl.when(jnp.logical_not(lower) & (chip < n_chip - 1))
    def _():
        pass_on(-1, True)

    tile_load.wait()

    def place_row(i, carry):
        rows = pl.ds(pl.multiple_of(i * tile, tile), tile)
        for t in range(tile_cols):
            at = (t % blocks) * (tile_cols // blocks) + t // blocks
            slot = jnp.clip(inverse_ref[0, i * tile_cols + t], 0, slots)
            dense[rows, at * tile : (at + 1) * tile] = tiles[slot]
        return carry

    lax.fori_loop(0, tile_rows, place_row, 0)
    for b in range(blocks):
        gather_start(0, b, 1)

    @pl.when(lower)
    def _():
        pass_on(-1, True)

    @pl.when(jnp.logical_not(lower))
    def _():
        pass_on(1, True)

    for load in weight_loads:
        load.wait()

    middle = jnp.where(end_chip, units, units // 2)
    run_first(0)
    run_merge(0)
    run_rest(0, 0, middle)
    if blocks > 1:
        settle(0, 0)
        hide(0)
        for h in range(known_parts):
            gather_start(1, 0, h)
    run_rest(0, middle, units)
    settle(0, blocks - 1)
    hide(blocks - 1)
    gather_start(1, blocks - 1, 0)
    gather_start(1, blocks - 1, 1)
    if blocks > 1:
        for h in range(known_parts):
            gather_wait(1, 0, h)
        for i in range(n_chip):
            early_unit(i)

    run_first(1)
    run_merge(1)
    run_rest(1, 0, middle)
    drain(0)
    if blocks > 1:
        settle(1, 0)
        out_ref[0:sub, :] = project(1, 0)
    run_rest(1, middle, units)
    drain(1)
    settle(1, blocks - 1)
    out_ref[(blocks - 1) * sub :, :] = project(1, blocks - 1)


def shards(n_row, n_col, features, tile_values, tile_places, tile_counts, weight_one, weight_two):
    tiles = tile_values.reshape(tile_values.shape[2:])
    places = tile_places.reshape(tile_places.shape[2:])
    slots, tile = tiles.shape[0], tiles.shape[1]
    piece, width = features.shape
    part = width // PARTS
    blocks = 2 if piece == 2 * tile else 1
    sub = piece // blocks
    rows, depth = piece * n_col, piece * n_row
    tile_rows, tile_cols = rows // tile, depth // tile
    n_chip = n_col // 2
    spots = tile_rows * tile_cols
    items = blocks * PARTS * n_chip
    detours = max(1, (blocks - 1) * PARTS * (n_chip - 2 if n_chip > 3 else n_chip))

    def flow(layer, count):
        return pltpu.VMEM((count, sub, part), LINK_TYPES[layer])

    def scales(count):
        return pltpu.VMEM((count, 1, part), jnp.float32)

    dma = pltpu.SemaphoreType.DMA
    hbm = pl.BlockSpec(memory_space=pltpu.HBM)
    second = pl.pallas_call(
        functools.partial(kernel, n_row, n_col, blocks),
        out_shape=jax.ShapeDtypeStruct((piece, width), jnp.float32),
        in_specs=[hbm] * 6,
        out_specs=pl.BlockSpec(memory_space=pltpu.VMEM),
        scratch_shapes=[
            pltpu.VMEM((slots + 1, tile, tile), jnp.bfloat16),
            pltpu.VMEM((rows, depth), jnp.bfloat16),
            pltpu.VMEM((2, width, width), jnp.float32),
            pltpu.VMEM((2, PARTS, depth, part), jnp.bfloat16),
            pltpu.VMEM((blocks, sub, width), jnp.float32),
            pltpu.VMEM((2, PARTS, n_chip, 2, piece, part), jnp.float32),
            pltpu.VMEM((2, PARTS, n_chip, piece, part), jnp.float32),
            flow(0, items), flow(1, items), flow(0, items), flow(1, items),
            flow(0, detours), flow(1, detours),
            scales(items), scales(items), scales(detours),
            pltpu.SemaphoreType.REGULAR((2,)), dma((6,)), dma(()),
            dma((2,)), dma((2, blocks, PARTS)),
            dma((2,)), dma((2, PARTS, n_chip)),
            dma((2,)), dma((2, 1 + (blocks - 1) * n_chip)), dma((2, detours)),
            dma(()), dma((1 + (blocks - 1) * n_chip,)), dma((detours,)),
            pltpu.SMEM(tile_counts.shape, jnp.int32), pltpu.VMEM(places.shape, jnp.int32),
            pltpu.VMEM((8, spots), jnp.int32), pltpu.SMEM((8, spots), jnp.int32),
        ],
        compiler_params=pltpu.CompilerParams(
            collective_id=0, has_side_effects=True, vmem_limit_bytes=40 * 1024 * 1024
        ),
    )(*(
        pltpu.with_memory_space_constraint(x, pltpu.HBM)
        for x in (tile_counts, places, features, tiles, weight_one, weight_two)
    ))
    return jnp.maximum(second, 0.0)


def solution(mesh):
    placed = (
        P(("row", "col"), None),
        P("row", "col", None, None, None),
        P("row", "col", None, None),
        P(),
        P(),
        P(),
    )
    return jax.shard_map(
        functools.partial(shards, mesh.shape["row"], mesh.shape["col"]),
        mesh=mesh, in_specs=placed, out_specs=P(("row", "col"), None), check_vma=False,
    )
```
